32 devices in a mesh: task: 2 (over core), row: 16 (over z, y, x).
Axes of the slice: x: 2, y: 2, z: 4, core: 2. Of those that a mesh axis runs over, the one named last changes fastest.
Arguments:
- activation_grams: float32 [2, 7168, 7168], P('task', 'row'), may hold values from -240 to 240, as said below
- adjusted_weights: bfloat16 [2, 7168, 2048], P('task', 'row'), may hold values from -0.59765625 to 0.59765625
Outputs:
- reduced_gram: float32 [7168, 7168], P('row')
- reduced_rhs: float32 [7168, 2048], P('row')
The draws below stay inside these ranges and needn't reach their ends.
Inputs may be any that keep to these rules, and one draw needn't show every extreme that they name: Each activation_grams[m] is symmetric and positive definite.
All inputs are finite; a program needn't handle non-finite values.
Results may differ from the reference program's by a relative error of at most 0.0003.
Values may be sent and summed in bfloat16 or wider, within the bound.
A program may use at most 192 MiB of HBM per device.

```python
import math
import jax
import jax.numpy as jnp
from jax import lax

H = 7168
DC = 2048
MODELS = 2
PANEL_STEPS = 2
N_ROW = 16


def draw_activation_grams(key, part):
    loading_key, scale_key = jax.random.split(jax.random.fold_in(key, 11))
    strong_rank = 8
    broad_rank = H + 1024
    base_share = 0.25
    strong_share = 0.5
    broad_share = 0.25
    spread_log = math.log(10.0)
    column_scale = jnp.concatenate([jnp.full((strong_rank,), math.sqrt(strong_share / strong_rank), jnp.float32), jnp.full((broad_rank,), math.sqrt(broad_share / broad_rank), jnp.float32)])

    def one_model(model_key):
        loadings = jax.random.normal(model_key, (H, strong_rank + broad_rank), jnp.float32) * column_scale
        shared = jnp.dot(loadings, loadings.T, precision=lax.Precision.HIGHEST)
        return 0.5 * (shared + shared.T)
    common = lax.map(one_model, jax.random.split(loading_key, MODELS))
    correlated = common + base_share * jnp.eye(H, dtype=jnp.float32)
    position = jnp.arange(H, dtype=jnp.float32) / H
    roughness = jnp.exp(jax.random.uniform(scale_key, (MODELS, H), jnp.float32, 0.0, spread_log))
    rooted = jnp.sqrt(roughness * jnp.exp(math.log(3.0) * position))
    return (rooted[:, :, None] * correlated * rooted[:, None, :]).astype(jnp.float32)


def block_levels(key, shape, pieces, low, largest):
    def one(dim, shards_of):
        steps = jax.random.uniform(jax.random.fold_in(jax.random.fold_in(key, 6), dim), (shards_of,), jnp.float32, low / len(pieces), largest / len(pieces))
        return jnp.repeat(jnp.exp(steps), shape[dim] // shards_of).reshape((-1,) + (1,) * (len(shape) - dim - 1))

    loudness = one(*pieces[0])
    for cut in pieces[1:]:
        loudness = loudness * one(*cut)
    return loudness


def gaussian(stream_key, extent, scale, most, pieces=(), held_as=jnp.bfloat16):
    values = scale * jax.random.normal(stream_key, extent, jnp.float32)
    if pieces:
        values = values * block_levels(stream_key, extent, pieces, -0.22, 0.18)
    return jnp.clip(values, -most, most).astype(held_as)


def setup_inputs(seed: int = 0) -> dict:
    arg_keys = jax.random.split(jax.random.key(seed), 3)
    activation_grams = draw_activation_grams(jax.random.fold_in(arg_keys[2], 71), 0)
    adjusted_weights = gaussian(arg_keys[1], (MODELS, H, DC), 0.1, 0.59765625, ((0, 2), (1, 16)))
    return {"activation_grams": activation_grams, "adjusted_weights": adjusted_weights}


def reference(activation_grams, adjusted_weights):
    rows = H // N_ROW
    merged = jnp.zeros((H, H), jnp.float32)
    rhs = jnp.zeros((H, DC), jnp.float32)
    for model in range(MODELS):
        gram = activation_grams[model]
        diagonal_entries = jnp.diagonal(gram)
        scaling = H / jnp.sum(diagonal_entries)
        regular = scaling * (0.9 * gram + 0.1 * jnp.diag(diagonal_entries))
        merged = merged + regular
        rhs = rhs + jnp.dot(regular, adjusted_weights[model].astype(jnp.float32), precision=lax.Precision.HIGHEST)
    for panel in range(PANEL_STEPS):
        low = panel * rows
        high = low + rows
        factor = jnp.linalg.cholesky(merged[low:high, low:high])
        upper = jax.scipy.linalg.solve_triangular(factor, merged[low:high], lower=True)
        solved = jax.scipy.linalg.solve_triangular(factor, rhs[low:high], lower=True)
        below = upper[:, high:].T
        merged = jnp.concatenate([merged[:low], upper, merged[high:] - jnp.dot(below, upper, precision=lax.Precision.HIGHEST)], axis=0)
        rhs = jnp.concatenate([rhs[:low], solved, rhs[high:] - jnp.dot(below, solved, precision=lax.Precision.HIGHEST)], axis=0)
    return (merged, rhs)
```

```python
import functools

import jax
import jax.numpy as jnp
from jax import lax
from jax.experimental import pallas as pl
from jax.experimental.pallas import tpu as pltpu
from jax.sharding import PartitionSpec as P

PANEL_STEPS = 2
MESH = pl.DeviceIdType.MESH
HIGHEST = lax.Precision.HIGHEST
NN = (((1,), (0,)), ((), ()))
NT = (((1,), (1,)), ((), ()))
TN = (((0,), (0,)), ((), ()))

TWO = (
    (100000, 110000, 120000, 200010, 210010, 220011, 230010, 300020, 310020, 320020, 330021, 400030, 410030, 430030),
    (100001, 110001, 120001, 200011, 210011, 220010, 230011, 300021, 310021, 320021, 330020, 400031, 410031, 430031),
    (100010, 110010, 121000, 200110, 210021, 220000, 230021, 300120, 310011, 320011, 330030, 400020, 410020, 431030),
    (100101, 111000, 121001, 200111, 210000, 220001, 230020, 300121, 310030, 320010, 330031, 400131, 411030, 431031),
    (100021, 110021, 120101, 200030, 210020, 221010, 230030, 300000, 310010, 320000, 331020, 400011, 410011, 430131),
    (100020, 111010, 121101, 200031, 210031, 221111, 230031, 300001, 310001, 320001, 331121, 400010, 411020, 431131),
    (100030, 110011, 121021, 200100, 211020, 220100, 230120, 300130, 311010, 320110, 330130, 400000, 410021, 431011),
    (100031, 110031, 211031, 231011, 311001, 321021, 400001, 410001),
    (100120, 111021, 211030, 231111, 311000, 321121, 400110, 411011),
    (100131, 111030, 230130, 320100, 400101, 411000),
)

ONE = (
    (100000, 110000, 120000, 200010, 210010, 220010, 230010, 300020, 310020, 320020, 330020, 400030, 410030, 430030),
    (100010, 110010, 200000, 210000, 220000, 230020, 300030, 310030, 320010, 330030, 400020, 410020),
    (100020, 110020, 200110, 211000, 220110, 230030, 300120, 311030, 320000, 330120, 400010, 410010),
    (100030, 111020, 121020, 200030, 210030, 221100, 231100, 300000, 310000, 321130, 331130, 400000, 411010, 431010),
    (100110, 111030, 221110, 230130, 320100, 331120, 400120, 411000),
)
SIDE, LINE, LANE, PAD = 2, 4, 128, 512


def decoded(table):
    rounds = []
    for codes in table:
        acts = []
        for code in codes:
            z, link, a, b, s, part = (int(c) for c in str(code))
            acts.append((z - 1, link, (a, b, s, part)))
        rounds.append(acts)
    return rounds


def landed(act):
    z, link, (a, b, s, part) = act
    if link == 0:
        return z, (1 - a, b, s, part)
    if link == 1:
        return z, (a, 1 - b, s, part)
    return (z + 1 if link == 2 else z - 1), (a, b, s, part)


def pair_order(rounds):
    orders, ready = [], []
    for z in range(LINE):
        last = {(b, s): -1 for b in range(SIDE) for s in range(LINE)}
        for k, acts in enumerate(rounds):
            for act in acts:
                to, (_, b, s, _) = landed(act)
                if to == z:
                    last[b, s] = k
        ranked = sorted(last, key=lambda pair: (last[pair], pair))
        orders.append(ranked)
        ready.append([last[pair] for pair in ranked])
    return orders, [max(r[i] for r in ready) for i in range(SIDE * LINE)]


def mm(left, right, dims=NN):
    return lax.dot_general(left, right, dims, precision=HIGHEST, preferred_element_type=jnp.float32)


def bf(left, right, dims=NN):
    return lax.dot_general(left, right, dims, preferred_element_type=jnp.float32)


def halves(value):
    high = value.astype(jnp.bfloat16)
    return high, (value - high.astype(jnp.float32)).astype(jnp.bfloat16)


def iota(shape, dim):
    return lax.broadcasted_iota(jnp.int32, shape, dim)


def kernel(
    g, gps, w, em, eo, fm, fo, wg, xg,
    gpv, gt, wv, trown, trs, sv, xs, xrv, xrp, xpk, zacc, zsend, zrecv, rsb, rt, cw, li, xpm, xpo, xp2, dref, bref, uref,
    ah, al, xh, xl, wt,
    wsend, wrecv, xsend, xrecv, rsend, rrecv, asend, arecv, local, tsem, dsend, drecv, esend, erecv, elocal, fsend, frecv, flocal,
):
    f32 = jnp.float32
    rows, width = g.shape
    columns = w.shape[1]
    nodes = trs.shape[0]
    half, pair = rows // 2, 2 * rows
    packed = xpk.shape[0]
    part_rows = packed // 2
    blocks = columns // LANE
    me = lax.axis_index("row")
    t = lax.axis_index("task")
    x, y, z = me % 2, (me // 2) % 2, me // 4
    two, one = decoded(TWO), decoded(ONE)
    last_one = len(one) - 1
    links = ((t, me + 1 - 2 * x), (t, me + 2 - 4 * y), (t, me + 4), (t, me - 4))
    partner = (1 - t, me)

    def node_of(chunk):
        a, b, s, _ = chunk
        return s * 4 + (y + b - 2 * b * y) * 2 + (x + a - 2 * a * x)

    def by_z(fn):
        for value in range(LINE):
            @pl.when(z == value)
            def _():
                fn(value)

    def remote(src, dst, send, recv, target):
        return pltpu.make_async_remote_copy(
            src_ref=src, dst_ref=dst, send_sem=send, recv_sem=recv, device_id=target, device_id_type=MESH
        )

    def w_slot(chunk):
        start = node_of(chunk) * rows + chunk[3] * half
        return wg.at[pl.ds(pl.multiple_of(start, half), half)]

    def x_slot(chunk):
        return xg.at[node_of(chunk), pl.ds(chunk[3] * part_rows, part_rows)]

    def a_slot(chunk):
        return rt.at[node_of(chunk)]

    def w_own(part):
        return w.at[pl.ds(part * half, half)]

    def x_own(part):
        return xpk.at[pl.ds(part * part_rows, part_rows)]

    phases = {
        "w": (two, w_slot, w_own, wsend, wrecv),
        "x": (two, x_slot, x_own, xsend, xrecv),
        "a": (one, a_slot, None, asend, arecv),
    }

    def send_copies(phase, k, value):
        rounds, slot, own, send, recv = phases[phase]
        copies = []
        for from_z, link, chunk in rounds[k]:
            if from_z != value:
                continue
            src = slot(chunk)
            if own is not None and chunk[:3] == (0, 0, value):
                src = own(chunk[3])
            copies.append(remote(src, slot(chunk), send.at[k, link], recv.at[k, link], links[link]))
        return copies

    def recv_copies(phase, k, value):
        rounds, slot, _, send, recv = phases[phase]
        copies = []
        for act in rounds[k]:
            to, chunk = landed(act)
            if to == value:
                copies.append(remote(slot(chunk), slot(chunk), send.at[k, act[1]], recv.at[k, act[1]], links[act[1]]))
        return copies

    def start(phase, k, value):
        for copy in send_copies(phase, k, value):
            copy.start()

    def arrive(phase, k, value):
        for copy in recv_copies(phase, k, value):
            copy.wait_recv()

    def sent(phase, k, value):
        for copy in send_copies(phase, k, value):
            copy.wait_send()

    back = (0, 1, 3, 2)

    def reduce_moves(k, value):
        out, come = [], []
        for act in one[last_one - k]:
            to, chunk = landed(act)
            if to == value:
                out.append((back[act[1]], chunk))
            if act[0] == value:
                come.append((back[act[1]], act[2]))
        return out, come

    def reduce_copies(k, value):
        return [
            remote(zacc.at[node_of(chunk)], rsb.at[k, link], rsend.at[k, link], rrecv.at[k, link], links[link])
            for link, chunk in reduce_moves(k, value)[0]
        ]

    def reduce_start(k, value):
        for copy in reduce_copies(k, value):
            copy.start()

    def reduce_arrive(k, value):
        for link, chunk in reduce_moves(k, value)[1]:
            remote(rsb.at[k, link], rsb.at[k, link], rsend.at[k, link], rrecv.at[k, link], links[link]).wait_recv()
            owner = node_of(chunk)
            zacc[owner] = zacc[owner] + rsb[k, link]

    def reduce_sent(k, value):
        for copy in reduce_copies(k, value):
            copy.wait_send()

    by_z(lambda v: start("w", 0, v))
    copy_gps = pltpu.make_async_copy(gps, gpv, local.at[0])
    own_pair = pl.ds(pl.multiple_of((me // 2) * pair, LANE), pair)
    copy_diag = pltpu.make_async_copy(g.at[:, own_pair], gt.at[0], local.at[1])
    copy_w = pltpu.make_async_copy(w, wv, local.at[2])
    copy_diag.start()
    copy_gps.start()
    copy_w.start()
    copy_diag.wait()
    on_diag = iota((rows, pair), 1) == iota((rows, pair), 0) + rows * (me % 2)
    trace = jnp.sum(jnp.where(on_diag, gt[0], 0.0), keepdims=True)
    trown[...] = jnp.broadcast_to(trace, trown.shape)
    trs[me] = jnp.broadcast_to(trace, trown.shape)
    trace_copies = [
        remote(trown, trs.at[me], tsem.at[0], tsem.at[1], (t, (me + k) % nodes)) for k in range(1, nodes)
    ]
    for copy in trace_copies:
        copy.start()
    others = trs.at[pl.ds(0, nodes - 1)]
    remote(others, others, tsem.at[0], tsem.at[1], partner).wait_recv()
    total = jnp.sum(trs[...], axis=0)[0:1, 0:1]
    scale = width / total
    sv[...] = jnp.broadcast_to(scale, sv.shape)

    copy_gps.wait()

    def panel(which):
        raw = gpv[which]
        eye = (iota((rows, rows), 0) == iota((rows, rows), 1)) & (me == which)
        return scale * (0.9 * raw + jnp.where(eye, 0.1 * raw, 0.0))

    xs[...] = panel(1 - t)
    swap = remote(xs, xrv, dsend.at[0], drecv.at[0], partner)
    swap.start()
    xrp[t] = jnp.zeros(xrp.shape[1:], f32)
    swap.wait_recv()
    xrp[t, :, 0:rows] = panel(t) + xrv[...]
    share = remote(xrp.at[t], xrp.at[t], dsend.at[1], drecv.at[1], partner)
    share.start()
    for h in range(2):
        for j in range(3):
            xpk[(3 * h + j) * half : (3 * h + j + 1) * half, :] = xrp[t, h * half : (h + 1) * half, j * LANE : (j + 1) * LANE]
    xpk[6 * half : 7 * half, :] = xrp[t, 0:half, 3 * LANE : PAD] + pltpu.roll(
        xrp[t, half:rows, 3 * LANE : PAD], LANE // 2, 1
    )
    store_x = pltpu.make_async_copy(xpk, xg.at[me], local.at[3])
    store_x.start()
    copy_w.wait()
    own_rows = pl.ds(pl.multiple_of(me * rows, rows), rows)
    store_w = pltpu.make_async_copy(wv, wg.at[own_rows], local.at[4])
    store_w.start()
    by_z(lambda v: (start("x", 0, v), start("x", 1, v)))

    def products(which, into):
        high, low = halves(panel(which))
        for c in range(columns // PAD):
            part = wv[:, c * PAD : (c + 1) * PAD]
            value = bf(high, part, TN) + bf(low, part, TN)
            for q in range(PAD // LANE):
                into[c * (PAD // LANE) + q] = value[:, q * LANE : (q + 1) * LANE]

    products(1 - t, zsend)
    trade = remote(zsend, zrecv, dsend.at[2], drecv.at[2], partner)
    trade.start()
    by_z(lambda v: (arrive("x", 0, v), start("x", 2, v)))
    products(t, zacc)
    by_z(lambda v: (arrive("x", 1, v), start("x", 3, v)))
    trade.wait()

    @pl.loop(0, blocks)
    def _(i):
        zacc[i] = zacc[i] + zrecv[i]

    for k in range(4, len(two)):
        by_z(lambda v: (arrive("x", k - 2, v), start("x", k, v)))

    share.wait()
    store_x.wait()
    store_w.wait()
    by_z(lambda v: (arrive("x", len(two) - 2, v), reduce_start(0, v), start("w", 1, v)))
    size = cw.shape[0]
    same = iota((size, size), 0) == iota((size, size), 1)
    li[...] = jnp.where(same, 1.0, 0.0)
    cw[...] = jnp.where(same & (iota((size, size), 0) % PAD >= rows), 1.0, 0.0)
    by_z(lambda v: arrive("x", len(two) - 1, v))
    fetch = pltpu.make_async_copy(xg.at[pl.ds(0, 2)], xpm, local.at[5])
    fetch.start()
    fetch.wait()
    give = remote(xpm, xpo, dsend.at[3], drecv.at[3], partner)
    give.start()

    low_lanes = iota((half, LANE), 1) < LANE // 2

    def tile(ref, h, j):
        if j < 3:
            return ref[(3 * h + j) * half : (3 * h + j + 1) * half, :]
        last = ref[6 * half : 7 * half, :]
        if h == 1:
            last = pltpu.roll(last, LANE // 2, 1)
        return jnp.where(low_lanes, last, 0.0)

    def place(ref, which):
        for k in range(2):
            for h in range(2):
                for j in range(4):
                    at = pl.ds(pl.multiple_of(which * PAD + j * LANE, LANE), LANE)
                    cw[k * PAD + h * half : k * PAD + (h + 1) * half, at] = tile(ref.at[k], h, j)

    place(xpm, t)
    give.wait()
    place(xpo, 1 - t)

    def eliminate(k):
        o = k * LANE
        pivots = LANE // 2 if (k + 1) * LANE % PAD == 0 else LANE
        sub, lane = iota((LANE, LANE), 0), iota((LANE, LANE), 1)
        sub1, lane1 = iota((LANE, 1), 0), iota((1, LANE), 1)
        dref[...] = cw[o : o + LANE, o : o + LANE]
        bref[...] = jnp.where(sub == lane, 1.0, 0.0)

        def pivot(j, carry):
            d = dref[...]
            row, brow = dref[pl.ds(j, 1), :], bref[pl.ds(j, 1), :]
            inverse = 1.0 / jnp.sum(jnp.where(lane1 == j, row, 0.0), axis=1, keepdims=True)
            column = jnp.sum(jnp.where(lane == j, d, 0.0), axis=1, keepdims=True)
            factor = jnp.where(sub1 > j, column * inverse, 0.0)
            dref[...] = d - factor * row
            bref[...] = bref[...] - factor * brow
            return carry

        lax.fori_loop(0, pivots, pivot, 0)
        diagonal = jnp.sum(jnp.where(sub == lane, dref[...], 0.0), axis=1, keepdims=True)
        inverse = bref[...] * lax.rsqrt(diagonal)
        done = mm(inverse, li[o : o + LANE, 0 : o + LANE])
        li[o : o + LANE, 0 : o + LANE] = done
        if o + LANE < size:
            ahead = mm(inverse, cw[o : o + LANE, o + LANE : size])
            uref[:, o + LANE : size] = ahead

            def below(i, carry):
                at = pl.ds(pl.multiple_of(i * LANE, LANE), LANE)
                left = jnp.transpose(uref[:, at])
                cw[at, o + LANE : size] = cw[at, o + LANE : size] - mm(left, uref[:, o + LANE : size])
                li[at, 0 : o + LANE] = li[at, 0 : o + LANE] - mm(left, li[o : o + LANE, 0 : o + LANE])
                return carry

            lax.fori_loop(k + 1, size // LANE, below, 0)

    def coefficients():
        for c in range(size // 256):
            chunk = li[c * 256 : (c + 1) * 256, :]
            cw[0:rows, c * 256 : (c + 1) * 256] = mm(xrp[0], chunk[:, 0:PAD], NT) + mm(xrp[1], chunk[:, PAD:size], NT)
        top = pl.ds(pl.multiple_of(jnp.minimum(me, 1) * PAD, PAD), rows)
        for c in range(PAD // 256):
            at = pl.ds(pl.multiple_of(t * PAD + c * 256, 256), 256)
            lower = -mm(cw[0:rows, :], li[:, at])
            value = jnp.where(me < PANEL_STEPS, li[top, at], lower)
            ah[:, c * 256 : (c + 1) * 256], al[:, c * 256 : (c + 1) * 256] = halves(value)

    def own_block(ref, j):
        raw = ref[...]
        eye = iota((rows, pair), 1) + j * pair == iota((rows, pair), 0) + me * rows
        return sv[0:1, 0:1] * (0.9 * raw + jnp.where(eye, 0.1 * raw, 0.0))

    def gram_tile(j, slot, sem):
        return pltpu.make_async_copy(g.at[:, pl.ds(pl.multiple_of(j * pair, LANE), pair)], gt.at[slot], sem)

    def gram_pieces():
        def load(j, slot):
            return (
                gram_tile(j, slot, elocal.at[slot, 0]),
                pltpu.make_async_copy(xg.at[pl.ds(2 * j, 2)], xp2.at[slot], elocal.at[slot, 1]),
            )

        def out(j, slot):
            tile_out = cw.at[pl.ds(pl.multiple_of(slot * PAD, PAD), rows), pl.ds(0, pair)]
            at = pl.ds(pl.multiple_of(j * pair, LANE), pair)
            return (
                pltpu.make_async_copy(tile_out, em.at[:, at], elocal.at[slot, 2]),
                remote(tile_out, eo.at[:, at], esend.at[j], erecv.at[j], partner),
            )

        for copy in load(0, 0):
            copy.start()

        def piece(j, carry):
            slot = j % 2
            for copy in load(j, slot):
                copy.wait()

            @pl.when(j + 1 < blocks // 2)
            def _():
                for copy in load(j + 1, 1 - slot):
                    copy.start()

            @pl.when(j >= 2)
            def _():
                keep, away = out(j - 2, slot)
                keep.wait()
                away.wait()

            for k in range(2):
                for h in range(2):
                    at = slice(k * rows + h * half, k * rows + (h + 1) * half)
                    for q in range(4):
                        high, low = halves(tile(xp2.at[slot, k], h, q))
                        xh[at, q * LANE : (q + 1) * LANE] = high
                        xl[at, q * LANE : (q + 1) * LANE] = low
            value = bf(ah[...], xh[...], NT) + (bf(ah[...], xl[...], NT) + bf(al[...], xh[...], NT))
            value = value + jnp.where(me >= PANEL_STEPS, own_block(gt.at[slot], j), 0.0)
            cw[pl.ds(pl.multiple_of(slot * PAD, PAD), rows), pl.ds(0, pair)] = value
            keep, away = out(j, slot)
            keep.start()
            away.start()
            return carry

        lax.fori_loop(0, blocks // 2, piece, 0)
        for j in (blocks // 2 - 2, blocks // 2 - 1):
            keep, away = out(j, j % 2)
            keep.wait()
            away.wait()

    orders, ready = pair_order(two)

    def weight_piece(position):
        b = [orders[v][position][0] for v in range(LINE)]
        s = [orders[v][position][1] for v in range(LINE)]

        def pick(values):
            chosen = values[LINE - 1]
            for v in range(LINE - 2, -1, -1):
                chosen = jnp.where(z == v, values[v], chosen)
            return chosen

        bb = pick(b)
        j = pick(s) * 2 + (y + bb - 2 * bb * y)
        slot = position % 2
        copies = [gram_tile(j, slot, local.at[6])]
        rows_of = pl.ds(pl.multiple_of(j * pair, pair), pair)
        for h in range(2):
            columns_of = pl.ds(h * (columns // 2), columns // 2)
            copies.append(pltpu.make_async_copy(wg.at[rows_of, columns_of], wt.at[h], local.at[7 + h]))
        for copy in copies:
            copy.start()
        copies[0].wait()
        high, low = halves(own_block(gt.at[slot], j))
        per = (columns // 2) // PAD
        for h in range(2):
            copies[1 + h].wait()
            for c in range(per):
                part = wt[h, :, c * PAD : (c + 1) * PAD]
                value = bf(high, part) + bf(low, part)
                for q in range(PAD // LANE):
                    at = (h * per + c) * (PAD // LANE) + q
                    piece = value[:, q * LANE : (q + 1) * LANE]
                    zsend[at] = piece if position == 0 else zsend[at] + piece

    eliminate(0)
    work = {1: (1, 2), 2: (3,), 3: (4, 5), 4: (6, 7)}
    for k in range(1, 5):
        by_z(lambda v: (reduce_arrive(k - 1, v), reduce_start(k, v), arrive("w", k - 1, v), start("w", k + 1, v)))
        for block in work[k]:
            eliminate(block)

    def own_top(v):
        reduce_arrive(4, v)
        rt[me] = zacc[me]
        start("a", 0, v)
        arrive("w", 4, v)
        start("w", 6, v)

    by_z(own_top)
    coefficients()
    weight_piece(0)
    weight_piece(1)
    by_z(lambda v: (arrive("a", 0, v), start("a", 1, v), arrive("w", 5, v), start("w", 7, v)))
    gram_pieces()
    by_z(lambda v: (arrive("a", 1, v), start("a", 2, v), arrive("w", 6, v), start("w", 8, v)))
    weight_piece(2)
    by_z(lambda v: (arrive("a", 2, v), start("a", 3, v), arrive("w", 7, v), start("w", 9, v)))
    weight_piece(3)
    weight_piece(4)
    by_z(lambda v: (arrive("a", 3, v), start("a", 4, v), arrive("w", 8, v)))
    weight_piece(5)
    weight_piece(6)
    by_z(lambda v: arrive("w", 9, v))
    weight_piece(7)
    by_z(lambda v: arrive("a", 4, v))

    group = blocks // 4

    def rhs_out(q):
        at = pl.ds(q * group, group)
        return (
            pltpu.make_async_copy(zsend.at[at], fm.at[at], flocal.at[q]),
            remote(zsend.at[at], fo.at[at], fsend.at[q], frecv.at[q], partner),
        )

    for q in range(4):
        for i in range(q * group, (q + 1) * group):
            high, low = halves(rt[i])
            left, rest = ah[:, 0:rows], al[:, 0:rows]
            value = bf(left, high) + (bf(left, low) + bf(rest, high))
            zsend[i] = jnp.where(me >= PANEL_STEPS, zsend[i], 0.0) + value
        for copy in rhs_out(q):
            copy.start()
    for q in range(4):
        for copy in rhs_out(q):
            copy.wait()

    for copy in trace_copies[:1]:
        remote(others, others, tsem.at[0], tsem.at[1], partner).wait_send()
    swap.wait_send()

    def finish(v):
        for k in range(len(two)):
            sent("w", k, v)
            sent("x", k, v)
        for k in range(len(one)):
            sent("a", k, v)
            reduce_sent(k, v)

    by_z(finish)


def fused(parts, activation_grams, adjusted_weights):
    f32, b16 = jnp.float32, jnp.bfloat16
    gram, weights = activation_grams[0], adjusted_weights[0]
    rows, width = gram.shape
    columns = weights.shape[1]
    half, blocks, size = rows // 2, columns // LANE, PANEL_STEPS * PAD
    packed = 7 * half
    gps = jnp.stack([gram[:, k * rows : (k + 1) * rows] for k in range(PANEL_STEPS)])
    hbm = pl.BlockSpec(memory_space=pl.ANY)
    vmem, dma = pltpu.VMEM, pltpu.SemaphoreType.DMA
    block = (blocks, rows, LANE)
    rounds, short = len(TWO), len(ONE)
    em, eo, fm, fo, _, _ = pl.pallas_call(
        kernel,
        out_shape=[
            jax.ShapeDtypeStruct((rows, width), f32),
            jax.ShapeDtypeStruct((rows, width), f32),
            jax.ShapeDtypeStruct(block, f32),
            jax.ShapeDtypeStruct(block, f32),
            jax.ShapeDtypeStruct((parts * rows, columns), b16),
            jax.ShapeDtypeStruct((parts, packed, LANE), f32),
        ],
        in_specs=[hbm] * 3,
        out_specs=[hbm] * 6,
        scratch_shapes=[
            vmem((2, rows, rows), f32), vmem((2, rows, 2 * rows), f32), vmem((rows, columns), b16),
            vmem((8, LANE), f32), vmem((parts, 8, LANE), f32), vmem((8, LANE), f32),
            vmem((rows, rows), f32), vmem((rows, rows), f32), vmem((2, rows, PAD), f32), vmem((packed, LANE), f32),
            vmem(block, f32), vmem(block, f32), vmem(block, f32), vmem((short, 4, rows, LANE), f32), vmem(block, f32),
            vmem((size, size), f32), vmem((size, size), f32),
            vmem((2, packed, LANE), f32), vmem((2, packed, LANE), f32), vmem((2, 2, packed, LANE), f32),
            vmem((LANE, LANE), f32), vmem((LANE, LANE), f32), vmem((LANE, size), f32),
            vmem((rows, PAD), b16), vmem((rows, PAD), b16), vmem((2 * rows, PAD), b16), vmem((2 * rows, PAD), b16),
            vmem((2, 2 * rows, columns // 2), b16),
            dma((rounds, 4)), dma((rounds, 4)), dma((rounds, 4)), dma((rounds, 4)),
            dma((short, 4)), dma((short, 4)), dma((short, 4)), dma((short, 4)),
            dma((9,)), dma((2,)), dma((4,)), dma((4,)), dma((8,)), dma((8,)), dma((2, 3)), dma((4,)), dma((4,)), dma((4,)),
        ],
        compiler_params=pltpu.CompilerParams(has_side_effects=True, vmem_limit_bytes=67043328),
        name="merge",
    )(gram, gps, weights)
    rhs = jnp.transpose(fm + fo, (1, 0, 2)).reshape(rows, columns)
    return em + eo, rhs


def product(left, right):
    return jnp.dot(left, right, precision=lax.Precision.HIGHEST)


def inverse_of(factor):
    identity = jnp.eye(factor.shape[0], dtype=factor.dtype)
    return jax.scipy.linalg.solve_triangular(factor, identity, lower=True)


def leading_block(columns_block, parts, rows, wide):
    position = lax.axis_index("row")
    holders = wide // rows
    if rows % parts == 0:
        pieces = lax.all_to_all(
            columns_block.reshape(parts, rows // parts, wide), "row", 0, 0, tiled=True
        )[:holders]
        gathered = lax.all_gather(pieces, "row", axis=1, tiled=True)
        return gathered.reshape(wide, wide)
    placed = jnp.zeros((wide, wide), columns_block.dtype)
    kept = jnp.where(position < holders, columns_block, 0)
    start = jnp.minimum(position, holders - 1) * rows
    return lax.psum(lax.dynamic_update_slice_in_dim(placed, kept, start, 0), "row")


def per_device(parts, activation_grams, adjusted_weights):
    gram = activation_grams[0]
    rows, width = gram.shape
    columns = adjusted_weights.shape[2]
    wide = PANEL_STEPS * rows
    position = lax.axis_index("row")
    task = lax.axis_index("task")
    start_col = position * rows
    weights = lax.all_gather(adjusted_weights[0], "row", axis=0, tiled=True)

    own_block = lax.dynamic_slice_in_dim(gram, start_col, rows, 1)
    diagonal_entries = jnp.diagonal(own_block)
    scaling = width / lax.psum(jnp.sum(diagonal_entries), "row")
    row_ids = lax.broadcasted_iota(jnp.int32, (rows, width), 0) + start_col
    col_ids = lax.broadcasted_iota(jnp.int32, (rows, width), 1)
    source = scaling * (0.9 * gram + jnp.where(row_ids == col_ids, 0.1 * gram, 0.0))

    panel_cols = lax.psum(source[:, :wide], "task")
    corner = leading_block(panel_cols, parts, rows, wide)
    first_inverse = inverse_of(jnp.linalg.cholesky(corner[:rows, :rows]))
    left = product(corner[rows:, :rows], first_inverse.T)
    second = jnp.linalg.cholesky(corner[rows:, rows:] - product(left, left.T))
    second_inverse = inverse_of(second)
    coupling = -product(second_inverse, product(left, first_inverse))
    solver = jnp.where(
        task == 0,
        jnp.concatenate([first_inverse, jnp.zeros_like(first_inverse)], axis=1),
        jnp.concatenate([coupling, second_inverse], axis=1),
    )
    mine = product(solver, panel_cols.T)
    upper = lax.all_gather(mine, "row", axis=1, tiled=True)

    high = lax.reduce_precision(source, 8, 7)
    low = (source - high).astype(jnp.bfloat16)
    folded = jnp.dot(
        high.astype(jnp.bfloat16), weights, preferred_element_type=jnp.float32
    ) + jnp.dot(low, weights, preferred_element_type=jnp.float32)

    pieces = lax.all_to_all(folded, "row", 1, 0, tiled=True)
    held, solver = lax.optimization_barrier((pieces[:wide], solver))
    top = lax.psum(held, "task")
    solved = lax.all_gather(product(solver, top), "row", axis=1, tiled=True)

    below = position >= PANEL_STEPS
    holds = position == task
    merged_part = jnp.where(
        below, source - product(mine.T, upper), jnp.where(holds, upper, 0.0)
    )
    rhs_part = jnp.where(
        below, folded - product(mine.T, solved), jnp.where(holds, solved, 0.0)
    )
    return lax.psum((merged_part, rhs_part), "task")


def solution(mesh):
    assert mesh.shape["task"] == PANEL_STEPS
    parts = mesh.shape["row"]
    placed = (P("task", "row", None), P("task", "row", None))

    def run(grams, weights):
        rows, columns = grams.shape[1], weights.shape[2]
        fits = parts == SIDE * SIDE * LINE and rows == 7 * LANE // 2 and columns == parts * LANE
        return (fused if fits else per_device)(parts, grams, weights)

    return jax.shard_map(
        run,
        mesh=mesh,
        in_specs=placed,
        out_specs=(P("row", None), P("row", None)),
        check_vma=False,
    )
```

```python
import functools

import jax
import jax.numpy as jnp
from jax import lax
from jax.experimental import pallas as pl
from jax.experimental.pallas import tpu as pltpu
from jax.sharding import PartitionSpec as P

PANEL_STEPS = 2
MESH = pl.DeviceIdType.MESH
HIGHEST = lax.Precision.HIGHEST
NN = (((1,), (0,)), ((), ()))
NT = (((1,), (1,)), ((), ()))
TN = (((0,), (0,)), ((), ()))

TWO = (
    (100000, 110000, 120000, 200010, 210010, 220011, 230010, 300020, 310020, 320020, 330021, 400030, 410030, 430030),
    (100001, 110001, 120001, 200011, 210011, 220010, 230011, 300021, 310021, 320021, 330020, 400031, 410031, 430031),
    (100010, 110010, 121000, 200110, 210021, 220000, 230021, 300120, 310011, 320011, 330030, 400020, 410020, 431030),
    (100101, 111000, 121001, 200111, 210000, 220001, 230020, 300121, 310030, 320010, 330031, 400131, 411030, 431031),
    (100021, 110021, 120101, 200030, 210020, 221010, 230030, 300000, 310010, 320000, 331020, 400011, 410011, 430131),
    (100020, 111010, 121101, 200031, 210031, 221111, 230031, 300001, 310001, 320001, 331121, 400010, 411020, 431131),
    (100030, 110011, 121021, 200100, 211020, 220100, 230120, 300130, 311010, 320110, 330130, 400000, 410021, 431011),
    (100031, 110031, 211031, 231011, 311001, 321021, 400001, 410001),
    (100120, 111021, 211030, 231111, 311000, 321121, 400110, 411011),
    (100131, 111030, 230130, 320100, 400101, 411000),
)

ONE = (
    (100000, 110000, 120000, 200010, 210010, 220010, 230010, 300020, 310020, 320020, 330020, 400030, 410030, 430030),
    (100010, 110010, 200000, 210000, 220000, 230020, 300030, 310030, 320010, 330030, 400020, 410020),
    (100020, 110020, 200110, 211000, 220110, 230030, 300120, 311030, 320000, 330120, 400010, 410010),
    (100030, 111020, 121020, 200030, 210030, 221100, 231100, 300000, 310000, 321130, 331130, 400000, 411010, 431010),
    (100110, 111030, 221110, 230130, 320100, 331120, 400120, 411000),
)
FIRST = (
    (100001, 110001, 120000, 200010, 210010, 220011, 230010, 300021, 310020, 320021, 330020, 400031, 410030, 430031),
    (100101, 110000, 120001, 200000, 210000, 220000, 230020, 300020, 310011, 320011, 331021, 400130, 411031, 430130),
    (100100, 110020, 121101, 200100, 210001, 220001, 231000, 300000, 310000, 320000, 330130, 400011, 410021, 431131),
    (100120, 110010, 121001, 200011, 211021, 220101, 231010, 300001, 311000, 320001, 331131, 400000, 410000, 431031),
    (100020, 111010, 121120, 200130, 211011, 220010, 231021, 300101, 310031, 321100, 330031, 400001, 410001, 430030),
    (101021, 111021, 121110, 201121, 211130, 220110, 231130, 300030, 311021, 320010, 330030, 400101, 411011, 431011),
    (101130, 111130, 120120, 201131, 210011, 221110, 231011, 300130, 311020, 321020, 331031, 400010, 410010, 431111),
    (101011, 111011, 200020, 221010, 231031, 320131, 330021, 400021, 411020, 430121),
    (101031, 111031, 230121, 320111, 401020, 411010),
    (101030, 110011, 230131, 321030, 400121, 410020),
)
SIDE, LINE, LANE, PAD = 2, 4, 128, 512


def decoded(table):
    rounds = []
    for codes in table:
        acts = []
        for code in codes:
            z, link, a, b, s, part = (int(c) for c in str(code))
            acts.append((z - 1, link, (a, b, s, part)))
        rounds.append(acts)
    return rounds


def landed(act):
    z, link, (a, b, s, part) = act
    if link == 0:
        return z, (1 - a, b, s, part)
    if link == 1:
        return z, (a, 1 - b, s, part)
    return (z + 1 if link == 2 else z - 1), (a, b, s, part)


def pair_order(rounds):
    orders, ready = [], []
    for z in range(LINE):
        last = {(b, s): -1 for b in range(SIDE) for s in range(LINE)}
        for k, acts in enumerate(rounds):
            for act in acts:
                to, (_, b, s, _) = landed(act)
                if to == z:
                    last[b, s] = k
        ranked = sorted(last, key=lambda pair: (last[pair], pair))
        orders.append(ranked)
        ready.append([last[pair] for pair in ranked])
    return orders, [max(r[i] for r in ready) for i in range(SIDE * LINE)]


def mm(left, right, dims=NN):
    return lax.dot_general(left, right, dims, precision=HIGHEST, preferred_element_type=jnp.float32)


def bf(left, right, dims=NN):
    return lax.dot_general(left, right, dims, preferred_element_type=jnp.float32)


def halves(value):
    high = value.astype(jnp.bfloat16)
    return high, (value - high.astype(jnp.float32)).astype(jnp.bfloat16)


def iota(shape, dim):
    return lax.broadcasted_iota(jnp.int32, shape, dim)


def kernel(
    g, w, em, eo, fm, fo, wg, xg,
    gpa, gpv, gt, wv, trown, trs, sv, xs, xrv, xrp, xpk, zacc, zsend, zrecv, rsb, rt, cw, li, xpm, xpo, xp2, dref, bref, cref, uref,
    ahl, xh, xl, rhl, wt,
    wsend, wrecv, xsend, xrecv, rsend, rrecv, asend, arecv, local, tsem, dsend, drecv, esend, erecv, elocal, fsend, frecv, flocal, wsem,
):
    f32 = jnp.float32
    rows, width = g.shape
    columns = w.shape[1]
    nodes = trs.shape[0]
    half, pair = rows // 2, 2 * rows
    packed = xpk.shape[0]
    part_rows = packed // 2
    blocks = columns // LANE
    me = lax.axis_index("row")
    t = lax.axis_index("task")
    x, y, z = me % 2, (me // 2) % 2, me // 4
    two, one, early = decoded(TWO), decoded(ONE), decoded(FIRST)
    last_one = len(one) - 1
    links = ((t, me + 1 - 2 * x), (t, me + 2 - 4 * y), (t, me + 4), (t, me - 4))
    partner = (1 - t, me)

    def node_of(chunk):
        a, b, s, _ = chunk
        return s * 4 + (y + b - 2 * b * y) * 2 + (x + a - 2 * a * x)

    def by_z(fn):
        for value in range(LINE):
            @pl.when(z == value)
            def _():
                fn(value)

    def remote(src, dst, send, recv, target):
        return pltpu.make_async_remote_copy(
            src_ref=src, dst_ref=dst, send_sem=send, recv_sem=recv, device_id=target, device_id_type=MESH
        )

    def w_slot(chunk):
        start = node_of(chunk) * rows + chunk[3] * half
        return wg.at[pl.ds(pl.multiple_of(start, half), half)]

    def x_slot(chunk):
        start = node_of(chunk) * packed + chunk[3] * part_rows
        return xg.at[pl.ds(pl.multiple_of(start, 8), part_rows)]

    def a_slot(chunk):
        return rt.at[node_of(chunk)]

    def w_own(part):
        return w.at[pl.ds(part * half, half)]

    def x_own(part):
        return xpk.at[pl.ds(part * part_rows, part_rows)]

    phases = {
        "w": (two, w_slot, w_own, wsend, wrecv),
        "x": (early, x_slot, x_own, xsend, xrecv),
        "a": (one, a_slot, None, asend, arecv),
    }

    def send_copies(phase, k, value):
        rounds, slot, own, send, recv = phases[phase]
        copies = []
        for from_z, link, chunk in rounds[k]:
            if from_z != value:
                continue
            src = slot(chunk)
            if own is not None and chunk[:3] == (0, 0, value):
                src = own(chunk[3])
            copies.append(remote(src, slot(chunk), send.at[k // 4, link], recv.at[k, link], links[link]))
        return copies

    def recv_copies(phase, k, value):
        rounds, slot, _, send, recv = phases[phase]
        copies = []
        for act in rounds[k]:
            to, chunk = landed(act)
            if to == value:
                copies.append(remote(slot(chunk), slot(chunk), send.at[k // 4, act[1]], recv.at[k, act[1]], links[act[1]]))
        return copies

    def start(phase, k, value):
        for copy in send_copies(phase, k, value):
            copy.start()

    def arrive(phase, k, value):
        for copy in recv_copies(phase, k, value):
            copy.wait_recv()

    back = (0, 1, 3, 2)

    def reduce_moves(k, value):
        out, come = [], []
        for act in one[last_one - k]:
            to, chunk = landed(act)
            if to == value:
                out.append((back[act[1]], chunk))
            if act[0] == value:
                come.append((back[act[1]], act[2]))
        return out, come

    def reduce_copies(k, value):
        return [
            remote(zacc.at[node_of(chunk)], rsb.at[k, link], rsend.at[link], rrecv.at[k, link], links[link])
            for link, chunk in reduce_moves(k, value)[0]
        ]

    def reduce_start(k, value):
        for copy in reduce_copies(k, value):
            copy.start()

    def reduce_arrive(k, value):
        for link, chunk in reduce_moves(k, value)[1]:
            remote(rsb.at[k, link], rsb.at[k, link], rsend.at[link], rrecv.at[k, link], links[link]).wait_recv()
            owner = node_of(chunk)
            zacc[owner] = zacc[owner] + rsb[k, link]

    copy_panels = pltpu.make_async_copy(g.at[:, pl.ds(0, pair)], gpa, local.at[0])
    own_pair = pl.ds(pl.multiple_of((me // 2) * pair, LANE), pair)
    copy_diag = pltpu.make_async_copy(g.at[:, own_pair], gt.at[0], local.at[1])
    copy_w = pltpu.make_async_copy(w, wv, local.at[2])
    copy_diag.start()
    copy_panels.start()
    copy_w.start()
    copy_diag.wait()
    on_diag = iota((rows, pair), 1) == iota((rows, pair), 0) + rows * (me % 2)
    trace = jnp.sum(jnp.where(on_diag, gt[0], 0.0), keepdims=True)
    trown[...] = jnp.broadcast_to(trace, trown.shape)
    trs[me] = jnp.broadcast_to(trace, trown.shape)
    trace_copies = [
        remote(trown, trs.at[me], tsem.at[0], tsem.at[1], (t, (me + k) % nodes)) for k in range(1, nodes)
    ]
    for copy in trace_copies:
        copy.start()
    by_z(lambda v: start("w", 0, v))
    copy_panels.wait()
    gpv[0] = gpa[:, 0:rows]
    gpv[1] = gpa[:, rows:pair]
    others = trs.at[pl.ds(0, nodes - 1)]
    remote(others, others, tsem.at[0], tsem.at[1], partner).wait_recv()
    total = jnp.sum(trs[...], axis=0)[0:1, 0:1]
    scale = width / total
    sv[...] = jnp.broadcast_to(scale, sv.shape)

    def panel(which):
        raw = gpv[which]
        eye = (iota((rows, rows), 0) == iota((rows, rows), 1)) & (me == which)
        return scale * (0.9 * raw + jnp.where(eye, 0.1 * raw, 0.0))

    xs[...] = panel(1 - t)
    swap = remote(xs, xrv, dsend.at[0], drecv.at[0], partner)
    swap.start()
    xrp[t] = jnp.zeros(xrp.shape[1:], f32)
    swap.wait_recv()
    xrp[t, :, 0:rows] = panel(t) + xrv[...]
    share = remote(xrp.at[t], xrp.at[t], dsend.at[1], drecv.at[1], partner)
    share.start()
    for h in range(2):
        for j in range(3):
            xpk[(3 * h + j) * half : (3 * h + j + 1) * half, :] = xrp[t, h * half : (h + 1) * half, j * LANE : (j + 1) * LANE]
    xpk[6 * half : 7 * half, :] = xrp[t, 0:half, 3 * LANE : PAD] + pltpu.roll(
        xrp[t, half:rows, 3 * LANE : PAD], LANE // 2, 1
    )
    own_x = pl.ds(pl.multiple_of(me * packed, 8), packed)
    store_x = pltpu.make_async_copy(xpk, xg.at[own_x], local.at[3])
    store_x.start()
    copy_w.wait()
    own_rows = pl.ds(pl.multiple_of(me * rows, rows), rows)
    store_w = pltpu.make_async_copy(wv, wg.at[own_rows], local.at[4])
    store_w.start()
    by_z(lambda v: start("x", 0, v))

    def products(which, into):
        high, low = halves(panel(which))
        xh[0:rows, 0:rows] = high
        xl[0:rows, 0:rows] = low

        @pl.loop(0, columns // PAD)
        def _(c):
            part = wv[:, pl.ds(pl.multiple_of(c * PAD, PAD), PAD)]
            value = bf(xh[0:rows, 0:rows], part, TN) + bf(xl[0:rows, 0:rows], part, TN)
            for q in range(PAD // LANE):
                into[c * (PAD // LANE) + q] = value[:, q * LANE : (q + 1) * LANE]

    products(1 - t, zsend)
    trade = remote(zsend, zrecv, dsend.at[2], drecv.at[2], partner)
    trade.start()
    by_z(lambda v: (arrive("x", 0, v), start("x", 1, v)))
    products(t, zacc)
    trade.wait()

    @pl.loop(0, blocks)
    def _(i):
        zacc[i] = zacc[i] + zrecv[i]

    def own_top(v):
        reduce_arrive(last_one, v)
        rt[me] = zacc[me]
        start("a", 0, v)

    by_z(lambda v: (arrive("x", 1, v), start("x", 2, v), reduce_start(0, v)))
    size = cw.shape[0]
    same = iota((size, size), 0) == iota((size, size), 1)
    li[...] = jnp.where(same, 1.0, 0.0)
    cw[...] = jnp.where(same & (iota((size, size), 0) % PAD >= rows), 1.0, 0.0)
    share.wait()
    store_x.wait()
    store_w.wait()
    for k in range(3, 6):
        by_z(
            lambda v, k=k: (
                arrive("x", k - 1, v), start("x", k, v), reduce_arrive(k - 3, v), reduce_start(k - 2, v)
            )
        )

    by_z(lambda v: (arrive("x", 5, v), start("x", 6, v)))
    fetch = pltpu.make_async_copy(xg.at[pl.ds(0, 2 * packed)], xpm, local.at[5])
    fetch.start()
    fetch.wait()
    give = remote(xpm, xpo, dsend.at[3], drecv.at[3], partner)
    give.start()

    low_lanes = iota((half, LANE), 1) < LANE // 2

    def tile(ref, h, j):
        if j < 3:
            return ref[(3 * h + j) * half : (3 * h + j + 1) * half, :]
        last = ref[6 * half : 7 * half, :]
        if h == 1:
            last = pltpu.roll(last, LANE // 2, 1)
        return jnp.where(low_lanes, last, 0.0)

    def place(ref, which):
        for k in range(2):
            for h in range(2):
                for j in range(4):
                    at = pl.ds(pl.multiple_of(which * PAD + j * LANE, LANE), LANE)
                    cw[k * PAD + h * half : k * PAD + (h + 1) * half, at] = tile(ref.at[k * packed : (k + 1) * packed], h, j)

    place(xpm, t)
    give.wait()
    place(xpo, 1 - t)

    def eliminate(k):
        o = pl.multiple_of(k * LANE, LANE)
        step, wide = 16, 2 * LANE
        own = pl.ds(o, LANE)
        groups = LANE // step - (LANE // step // 2) * ((k % 4) // 3)
        sub, lane, sub1 = iota((LANE, LANE), 0), iota((LANE, LANE), 1), iota((LANE, 1), 0)
        sub8, lane8 = iota((step, LANE), 0), iota((step, LANE), 1)
        dref[...] = cw[own, own]
        bref[...] = jnp.where(sub == lane, 1.0, 0.0)

        def pivots(i, carry):
            at = pl.multiple_of(i * step, step)
            here = pl.ds(at, step)
            rows8 = dref[here, :]
            for s in range(step):
                column = jnp.sum(jnp.where(lane8 == at + s, rows8, 0.0), axis=1, keepdims=True)
                cref[s, 0:step, :] = jnp.broadcast_to(column, (step, LANE))
            scaled = []
            for s in range(step):
                inverse = 1.0 / cref[s, s : s + 1, :]
                factor = jnp.where(sub8 > s, cref[s, 0:step, :] * inverse, 0.0)
                for later in range(s + 1, step):
                    cref[later, 0:step, :] = cref[later, 0:step, :] - factor * cref[later, s : s + 1, :]
                row, brow = dref[pl.ds(at + s, 1), :], bref[pl.ds(at + s, 1), :]
                dref[here, :] = dref[here, :] - factor * row
                bref[here, :] = bref[here, :] - factor * brow
                scaled.append(row * inverse)
            factors = jnp.transpose(jnp.concatenate(scaled * (LANE // step), axis=0))
            d, b = dref[...], bref[...]
            for s in range(step):
                factor = jnp.where(sub1 >= at + step, factors[:, s : s + 1], 0.0)
                d = d - factor * dref[pl.ds(at + s, 1), :]
                b = b - factor * bref[pl.ds(at + s, 1), :]
            dref[...] = d
            bref[...] = b
            return carry

        lax.fori_loop(0, groups, pivots, 0)
        diagonal = jnp.sum(jnp.where(sub == lane, dref[...], 0.0), axis=1, keepdims=True)
        bref[...] = bref[...] * lax.rsqrt(diagonal)
        first = (o + LANE) // wide
        last = (o + LANE + wide - 1) // wide
        count = size // wide

        def finish(n, carry):
            at = pl.ds(pl.multiple_of(n * wide, wide), wide)
            li[own, at] = mm(bref[...], li[own, at])
            return carry

        def ahead(n, carry):
            at = pl.ds(pl.multiple_of(n * wide, wide), wide)
            uref[:, at] = mm(bref[...], cw[own, at])
            return carry

        lax.fori_loop(0, last, finish, 0)
        lax.fori_loop(first, count, ahead, 0)

        def below(i, carry):
            at = pl.ds(pl.multiple_of(i * LANE, LANE), LANE)
            dref[...] = jnp.transpose(uref[:, at])

            def right(n, carry):
                to = pl.ds(pl.multiple_of(n * wide, wide), wide)
                cw[at, to] = cw[at, to] - mm(dref[...], uref[:, to])
                return carry

            def left(n, carry):
                to = pl.ds(pl.multiple_of(n * wide, wide), wide)
                li[at, to] = li[at, to] - mm(dref[...], li[own, to])
                return carry

            lax.fori_loop(first, count, right, 0)
            lax.fori_loop(0, last, left, 0)
            return carry

        lax.fori_loop(k + 1, size // LANE, below, 0)

    def coefficients():
        wide = 2 * LANE

        @pl.loop(0, size // wide)
        def _(c):
            at = pl.ds(pl.multiple_of(c * wide, wide), wide)
            cw[0:rows, at] = mm(xrp[0], li[at, 0:PAD], NT) + mm(xrp[1], li[at, PAD:size], NT)

        top = pl.ds(pl.multiple_of(jnp.minimum(me, 1) * PAD, PAD), rows)

        @pl.loop(0, PAD // wide)
        def _(c):
            at = pl.ds(pl.multiple_of(t * PAD + c * wide, wide), wide)
            to = pl.ds(pl.multiple_of(c * wide, wide), wide)
            lower = -mm(cw[0:rows, :], li[:, at])
            value = jnp.where(me < PANEL_STEPS, li[top, at], lower)
            ahl[0:rows, to], ahl[rows:pair, to] = halves(value)

    def own_block(ref, j):
        raw = ref[...]
        eye = iota((rows, pair), 1) + j * pair == iota((rows, pair), 0) + me * rows
        return sv[0:1, 0:1] * (0.9 * raw + jnp.where(eye, 0.1 * raw, 0.0))

    def gram_tile(j, slot, sem):
        return pltpu.make_async_copy(g.at[:, pl.ds(pl.multiple_of(j * pair, LANE), pair)], gt.at[slot], sem)

    def gram_pieces():
        def load(j, slot):
            return (
                gram_tile(j, slot, elocal.at[slot, 0]),
                pltpu.make_async_copy(
                    xg.at[pl.ds(pl.multiple_of(2 * j * packed, 8), 2 * packed)], xp2.at[slot], elocal.at[slot, 1]
                ),
            )

        def out(j, slot):
            tile_out = cw.at[pl.ds(pl.multiple_of(slot * PAD, PAD), rows), pl.ds(0, pair)]
            at = pl.ds(pl.multiple_of(j * pair, LANE), pair)
            return (
                pltpu.make_async_copy(tile_out, em.at[:, at], elocal.at[slot, 2]),
                remote(tile_out, eo.at[:, at], esend.at[j], erecv.at[j], partner),
            )

        for copy in load(0, 0):
            copy.start()

        def piece(j, carry):
            slot = j % 2
            for copy in load(j, slot):
                copy.wait()

            @pl.when(j + 1 < blocks // 2)
            def _():
                for copy in load(j + 1, 1 - slot):
                    copy.start()

            @pl.when(j >= 2)
            def _():
                keep, away = out(j - 2, slot)
                keep.wait()
                away.wait()

            for k in range(2):
                for h in range(2):
                    at = slice(k * rows + h * half, k * rows + (h + 1) * half)
                    for q in range(4):
                        high, low = halves(tile(xp2.at[slot, k * packed : (k + 1) * packed], h, q))
                        xh[at, q * LANE : (q + 1) * LANE] = high
                        xl[at, q * LANE : (q + 1) * LANE] = low
            both = bf(ahl[...], xh[...], NT)
            value = both[0:rows] + (both[rows:pair] + bf(ahl[0:rows, :], xl[...], NT))
            value = value + jnp.where(me >= PANEL_STEPS, own_block(gt.at[slot], j), 0.0)
            cw[pl.ds(pl.multiple_of(slot * PAD, PAD), rows), pl.ds(0, pair)] = value
            keep, away = out(j, slot)
            keep.start()
            away.start()
            return carry

        lax.fori_loop(0, blocks // 2, piece, 0)
        for j in (blocks // 2 - 2, blocks // 2 - 1):
            keep, away = out(j, j % 2)
            keep.wait()
            away.wait()

    orders, ready = pair_order(two)

    def weight_piece(position, arrived=lambda: None):
        b = [orders[v][position][0] for v in range(LINE)]
        s = [orders[v][position][1] for v in range(LINE)]

        def pick(values):
            chosen = values[LINE - 1]
            for v in range(LINE - 2, -1, -1):
                chosen = jnp.where(z == v, values[v], chosen)
            return chosen

        bb = pick(b)
        j = pick(s) * 2 + (y + bb - 2 * bb * y)
        load = gram_tile(j, position % 2, local.at[6])
        load.start()
        load.wait()
        high, low = halves(jnp.where(me >= PANEL_STEPS, own_block(gt.at[position % 2], j), 0.0))
        rhl[0:rows, :] = high
        rhl[rows:pair, :] = low
        arrived()
        rows_of = pl.ds(pl.multiple_of(j * pair, pair), pair)

        def part_copy(c):
            at = pl.ds(pl.multiple_of(c * PAD, PAD), PAD)
            return pltpu.make_async_copy(wg.at[rows_of, at], wt.at[c], wsem.at[c])

        for c in range(columns // PAD):
            part_copy(c).start()

        @pl.loop(0, columns // PAD)
        def _(c):
            part_copy(c).wait()
            both = bf(rhl[...], wt[c])
            value = both[0:rows] + both[rows:pair]
            for q in range(PAD // LANE):
                at = c * (PAD // LANE) + q
                piece = value[:, q * LANE : (q + 1) * LANE]
                zsend[at] = piece if position == 0 else zsend[at] + piece
            if position == SIDE * LINE - 1:
                for copy in rhs_out(c):
                    copy.start()

    def rhs_out(c):
        at = pl.ds(pl.multiple_of(c * (PAD // LANE), PAD // LANE), PAD // LANE)
        return (
            pltpu.make_async_copy(zsend.at[at], fm.at[at], flocal.at[c]),
            remote(zsend.at[at], fo.at[at], fsend.at[c], frecv.at[c], partner),
        )

    def top_share():
        @pl.loop(0, blocks)
        def _(i):
            high, low = halves(rt[i])
            both = bf(ahl[:, 0:rows], high)
            zsend[i] = zsend[i] + (both[0:rows] + (both[rows:pair] + bf(ahl[0:rows, 0:rows], low)))

    by_z(lambda v: (reduce_arrive(3, v), reduce_start(4, v), start("w", 1, v)))
    eliminate(0)
    by_z(lambda v: (arrive("x", 6, v), start("x", 7, v), own_top(v)))
    eliminate(1)
    by_z(lambda v: (arrive("x", 7, v), start("x", 8, v), arrive("a", 0, v), start("a", 1, v)))
    eliminate(2)
    by_z(lambda v: (arrive("x", 8, v), start("x", 9, v), arrive("a", 1, v), start("a", 2, v)))
    by_z(lambda v: (arrive("w", 0, v), start("w", 2, v)))
    lax.fori_loop(3, 5, lambda k, c: (eliminate(k), c)[1], 0)
    by_z(lambda v: (arrive("x", 9, v), arrive("a", 2, v), start("a", 3, v), arrive("w", 1, v), start("w", 3, v)))
    eliminate(5)
    by_z(lambda v: (arrive("a", 3, v), start("a", 4, v), arrive("w", 2, v), start("w", 4, v)))
    lax.fori_loop(6, 8, lambda k, c: (eliminate(k), c)[1], 0)
    by_z(lambda v: (arrive("w", 3, v), start("w", 5, v)))
    coefficients()
    gram_pieces()
    by_z(lambda v: (arrive("a", 4, v), arrive("w", 4, v), start("w", 6, v)))
    weight_piece(0)
    weight_piece(1)
    by_z(lambda v: (arrive("w", 5, v), start("w", 7, v)))
    weight_piece(2)
    top_share()
    by_z(lambda v: (arrive("w", 6, v), start("w", 8, v)))
    by_z(lambda v: (arrive("w", 7, v), start("w", 9, v)))
    weight_piece(3)
    weight_piece(4)
    weight_piece(5, lambda: by_z(lambda v: arrive("w", 8, v)))
    weight_piece(6)
    weight_piece(7, lambda: by_z(lambda v: arrive("w", 9, v)))
    for c in range(columns // PAD):
        for copy in rhs_out(c):
            copy.wait()

    for copy in trace_copies[:1]:
        remote(others, others, tsem.at[0], tsem.at[1], partner).wait_send()
    swap.wait_send()

    def drained(v):
        for link in range(4):
            for name, rounds, whole, rows_each in (("w", two, wg, half), ("x", early, xg, part_rows), ("a", one, rt, 1)):
                for first in range(0, len(rounds), 4):
                    count = sum(act[0] == v and act[1] == link for acts in rounds[first : first + 4] for act in acts)
                    sem = phases[name][3].at[first // 4, link]
                    if count:
                        all_of = whole.at[pl.ds(0, count * rows_each)]
                        remote(all_of, all_of, sem, sem, partner).wait_send()
            count = sum(move[0] == link for k in range(len(one)) for move in reduce_moves(k, v)[0])
            if count:
                all_of = zacc.at[pl.ds(0, count)]
                remote(all_of, all_of, rsend.at[link], rsend.at[link], partner).wait_send()

    by_z(drained)


def fused(parts, activation_grams, adjusted_weights):
    f32, b16 = jnp.float32, jnp.bfloat16
    gram, weights = activation_grams[0], adjusted_weights[0]
    rows, width = gram.shape
    columns = weights.shape[1]
    half, blocks, size = rows // 2, columns // LANE, PANEL_STEPS * PAD
    packed = 7 * half
    hbm = pl.BlockSpec(memory_space=pl.ANY)
    vmem, dma = pltpu.VMEM, pltpu.SemaphoreType.DMA
    block = (blocks, rows, LANE)
    rounds, short = len(TWO), len(ONE)
    em, eo, fm, fo, _, _ = pl.pallas_call(
        kernel,
        out_shape=[
            jax.ShapeDtypeStruct((rows, width), f32),
            jax.ShapeDtypeStruct((rows, width), f32),
            jax.ShapeDtypeStruct(block, f32),
            jax.ShapeDtypeStruct(block, f32),
            jax.ShapeDtypeStruct((parts * rows, columns), b16),
            jax.ShapeDtypeStruct((parts * packed, LANE), f32),
        ],
        in_specs=[hbm] * 2,
        out_specs=[hbm] * 6,
        scratch_shapes=[
            vmem((rows, 2 * rows), f32), vmem((2, rows, rows), f32), vmem((2, rows, 2 * rows), f32), vmem((rows, columns), b16),
            vmem((8, LANE), f32), vmem((parts, 8, LANE), f32), vmem((8, LANE), f32),
            vmem((rows, rows), f32), vmem((rows, rows), f32), vmem((2, rows, PAD), f32), vmem((packed, LANE), f32),
            vmem(block, f32), vmem(block, f32), vmem(block, f32), vmem((short, 4, rows, LANE), f32), vmem(block, f32),
            vmem((size, size), f32), vmem((size, size), f32),
            vmem((2 * packed, LANE), f32), vmem((2 * packed, LANE), f32), vmem((2, 2 * packed, LANE), f32),
            vmem((LANE, LANE), f32), vmem((LANE, LANE), f32), vmem((16, 16, LANE), f32), vmem((LANE, size), f32),
            vmem((2 * rows, PAD), b16), vmem((2 * rows, PAD), b16), vmem((2 * rows, PAD), b16),
            vmem((2 * rows, 2 * rows), b16), vmem((columns // PAD, 2 * rows, PAD), b16),
            dma((3, 4)), dma((rounds, 4)), dma((3, 4)), dma((rounds, 4)),
            dma((4,)), dma((short, 4)), dma((2, 4)), dma((short, 4)),
            dma((9,)), dma((2,)), dma((4,)), dma((4,)), dma((8,)), dma((8,)), dma((2, 3)), dma((4,)), dma((4,)), dma((4,)), dma((4,)),
        ],
        compiler_params=pltpu.CompilerParams(has_side_effects=True, vmem_limit_bytes=67043328),
        name="merge",
    )(gram, weights)
    rhs = jnp.transpose(fm + fo, (1, 0, 2)).reshape(rows, columns)
    return em + eo, rhs


def product(left, right):
    return jnp.dot(left, right, precision=lax.Precision.HIGHEST)


def inverse_of(factor):
    identity = jnp.eye(factor.shape[0], dtype=factor.dtype)
    return jax.scipy.linalg.solve_triangular(factor, identity, lower=True)


def leading_block(columns_block, parts, rows, wide):
    position = lax.axis_index("row")
    holders = wide // rows
    if rows % parts == 0:
        pieces = lax.all_to_all(
            columns_block.reshape(parts, rows // parts, wide), "row", 0, 0, tiled=True
        )[:holders]
        gathered = lax.all_gather(pieces, "row", axis=1, tiled=True)
        return gathered.reshape(wide, wide)
    placed = jnp.zeros((wide, wide), columns_block.dtype)
    kept = jnp.where(position < holders, columns_block, 0)
    start = jnp.minimum(position, holders - 1) * rows
    return lax.psum(lax.dynamic_update_slice_in_dim(placed, kept, start, 0), "row")


def per_device(parts, activation_grams, adjusted_weights):
    gram = activation_grams[0]
    rows, width = gram.shape
    columns = adjusted_weights.shape[2]
    wide = PANEL_STEPS * rows
    position = lax.axis_index("row")
    task = lax.axis_index("task")
    start_col = position * rows
    weights = lax.all_gather(adjusted_weights[0], "row", axis=0, tiled=True)

    own_block = lax.dynamic_slice_in_dim(gram, start_col, rows, 1)
    diagonal_entries = jnp.diagonal(own_block)
    scaling = width / lax.psum(jnp.sum(diagonal_entries), "row")
    row_ids = lax.broadcasted_iota(jnp.int32, (rows, width), 0) + start_col
    col_ids = lax.broadcasted_iota(jnp.int32, (rows, width), 1)
    source = scaling * (0.9 * gram + jnp.where(row_ids == col_ids, 0.1 * gram, 0.0))

    panel_cols = lax.psum(source[:, :wide], "task")
    corner = leading_block(panel_cols, parts, rows, wide)
    first_inverse = inverse_of(jnp.linalg.cholesky(corner[:rows, :rows]))
    left = product(corner[rows:, :rows], first_inverse.T)
    second = jnp.linalg.cholesky(corner[rows:, rows:] - product(left, left.T))
    second_inverse = inverse_of(second)
    coupling = -product(second_inverse, product(left, first_inverse))
    solver = jnp.where(
        task == 0,
        jnp.concatenate([first_inverse, jnp.zeros_like(first_inverse)], axis=1),
        jnp.concatenate([coupling, second_inverse], axis=1),
    )
    mine = product(solver, panel_cols.T)
    upper = lax.all_gather(mine, "row", axis=1, tiled=True)

    high = lax.reduce_precision(source, 8, 7)
    low = (source - high).astype(jnp.bfloat16)
    folded = jnp.dot(
        high.astype(jnp.bfloat16), weights, preferred_element_type=jnp.float32
    ) + jnp.dot(low, weights, preferred_element_type=jnp.float32)

    pieces = lax.all_to_all(folded, "row", 1, 0, tiled=True)
    held, solver = lax.optimization_barrier((pieces[:wide], solver))
    top = lax.psum(held, "task")
    solved = lax.all_gather(product(solver, top), "row", axis=1, tiled=True)

    below = position >= PANEL_STEPS
    holds = position == task
    merged_part = jnp.where(
        below, source - product(mine.T, upper), jnp.where(holds, upper, 0.0)
    )
    rhs_part = jnp.where(
        below, folded - product(mine.T, solved), jnp.where(holds, solved, 0.0)
    )
    return lax.psum((merged_part, rhs_part), "task")


def solution(mesh):
    assert mesh.shape["task"] == PANEL_STEPS
    parts = mesh.shape["row"]
    placed = (P("task", "row", None), P("task", "row", None))

    def run(grams, weights):
        rows, columns = grams.shape[1], weights.shape[2]
        fits = parts == SIDE * SIDE * LINE and rows == 7 * LANE // 2 and columns == parts * LANE
        return (fused if fits else per_device)(parts, grams, weights)

    return jax.shard_map(
        run,
        mesh=mesh,
        in_specs=placed,
        out_specs=(P("row", None), P("row", None)),
        check_vma=False,
    )
```

```python
import functools

import jax
import jax.numpy as jnp
from jax import lax
from jax.experimental import pallas as pl
from jax.experimental.pallas import tpu as pltpu
from jax.sharding import PartitionSpec as P

PANEL_STEPS = 2
MESH = pl.DeviceIdType.MESH
HIGHEST = lax.Precision.HIGHEST
NN = (((1,), (0,)), ((), ()))
NT = (((1,), (1,)), ((), ()))
TN = (((0,), (0,)), ((), ()))

TWO = (
    (100000, 110000, 120000, 200010, 210010, 220011, 230010, 300020, 310020, 320020, 330021, 400030, 410030, 430030),
    (100001, 110001, 120001, 200011, 210011, 220010, 230011, 300021, 310021, 320021, 330020, 400031, 410031, 430031),
    (100010, 110010, 121000, 200110, 210021, 220000, 230021, 300120, 310011, 320011, 330030, 400020, 410020, 431030),
    (100101, 111000, 121001, 200111, 210000, 220001, 230020, 300121, 310030, 320010, 330031, 400131, 411030, 431031),
    (100021, 110021, 120101, 200030, 210020, 221010, 230030, 300000, 310010, 320000, 331020, 400011, 410011, 430131),
    (100020, 111010, 121101, 200031, 210031, 221111, 230031, 300001, 310001, 320001, 331121, 400010, 411020, 431131),
    (100030, 110011, 121021, 200100, 211020, 220100, 230120, 300130, 311010, 320110, 330130, 400000, 410021, 431011),
    (100031, 110031, 211031, 231011, 311001, 321021, 400001, 410001),
    (100120, 111021, 211030, 231111, 311000, 321121, 400110, 411011),
    (100131, 111030, 230130, 320100, 400101, 411000),
)

ONE = (
    (100000, 110000, 120000, 200010, 210010, 220010, 230010, 300020, 310020, 320020, 330020, 400030, 410030, 430030),
    (100010, 110010, 200000, 210000, 220000, 230020, 300030, 310030, 320010, 330030, 400020, 410020),
    (100020, 110020, 200110, 211000, 220110, 230030, 300120, 311030, 320000, 330120, 400010, 410010),
    (100030, 111020, 121020, 200030, 210030, 221100, 231100, 300000, 310000, 321130, 331130, 400000, 411010, 431010),
    (100110, 111030, 221110, 230130, 320100, 331120, 400120, 411000),
)
FIRST = (
    (100001, 110001, 120000, 200010, 210010, 220011, 230010, 300021, 310020, 320021, 330020, 400031, 410030, 430031),
    (100101, 110000, 120001, 200000, 210000, 220000, 230020, 300020, 310011, 320011, 331021, 400130, 411031, 430130),
    (100100, 110020, 121101, 200100, 210001, 220001, 231000, 300000, 310000, 320000, 330130, 400011, 410021, 431131),
    (100120, 110010, 121001, 200011, 211021, 220101, 231010, 300001, 311000, 320001, 331131, 400000, 410000, 431031),
    (100020, 111010, 121120, 200130, 211011, 220010, 231021, 300101, 310031, 321100, 330031, 400001, 410001, 430030),
    (101021, 111021, 121110, 201121, 211130, 220110, 231130, 300030, 311021, 320010, 330030, 400101, 411011, 431011),
    (101130, 111130, 120120, 201131, 210011, 221110, 231011, 300130, 311020, 321020, 331031, 400010, 410010, 431111),
    (101011, 111011, 200020, 221010, 231031, 320131, 330021, 400021, 411020, 430121),
    (101031, 111031, 230121, 320111, 401020, 411010),
    (101030, 110011, 230131, 321030, 400121, 410020),
)
SIDE, LINE, LANE, PAD = 2, 4, 128, 512


def decoded(table):
    rounds = []
    for codes in table:
        acts = []
        for code in codes:
            z, link, a, b, s, part = (int(c) for c in str(code))
            acts.append((z - 1, link, (a, b, s, part)))
        rounds.append(acts)
    return rounds


def landed(act):
    z, link, (a, b, s, part) = act
    if link == 0:
        return z, (1 - a, b, s, part)
    if link == 1:
        return z, (a, 1 - b, s, part)
    return (z + 1 if link == 2 else z - 1), (a, b, s, part)


def pair_order(rounds):
    orders, ready = [], []
    for z in range(LINE):
        last = {(b, s): -1 for b in range(SIDE) for s in range(LINE)}
        for k, acts in enumerate(rounds):
            for act in acts:
                to, (_, b, s, _) = landed(act)
                if to == z:
                    last[b, s] = k
        ranked = sorted(last, key=lambda pair: (last[pair], pair))
        orders.append(ranked)
        ready.append([last[pair] for pair in ranked])
    return orders, [max(r[i] for r in ready) for i in range(SIDE * LINE)]


def mm(left, right, dims=NN):
    return lax.dot_general(left, right, dims, precision=HIGHEST, preferred_element_type=jnp.float32)


def bf(left, right, dims=NN):
    return lax.dot_general(left, right, dims, preferred_element_type=jnp.float32)


def halves(value):
    high = value.astype(jnp.bfloat16)
    return high, (value - high.astype(jnp.float32)).astype(jnp.bfloat16)


def iota(shape, dim):
    return lax.broadcasted_iota(jnp.int32, shape, dim)


def kernel(
    g, w, em, eo, fm, fo, wg, xg,
    gpa, gpv, gt, wv, trown, trs, sv, xs, xrv, xrp, xpk, zacc, zsend, zrecv, rsb, rt, cw, li, xpm, xpo, xp2, dref, bref, cref, uref,
    ahl, xh, xl, rhl, wt,
    wsend, wrecv, xsend, xrecv, rsend, rrecv, asend, arecv, local, tsem, dsend, drecv, esend, erecv, elocal, fsend, frecv, flocal, wsem,
):
    f32 = jnp.float32
    rows, width = g.shape
    columns = w.shape[1]
    nodes = trs.shape[0]
    half, pair = rows // 2, 2 * rows
    packed = xpk.shape[0]
    part_rows = packed // 2
    blocks = columns // LANE
    me = lax.axis_index("row")
    t = lax.axis_index("task")
    x, y, z = me % 2, (me // 2) % 2, me // 4
    two, one, early = decoded(TWO), decoded(ONE), decoded(FIRST)
    last_one = len(one) - 1
    links = ((t, me + 1 - 2 * x), (t, me + 2 - 4 * y), (t, me + 4), (t, me - 4))
    partner = (1 - t, me)

    def node_of(chunk):
        a, b, s, _ = chunk
        return s * 4 + (y + b - 2 * b * y) * 2 + (x + a - 2 * a * x)

    def by_z(fn):
        for value in range(LINE):
            @pl.when(z == value)
            def _():
                fn(value)

    def remote(src, dst, send, recv, target):
        return pltpu.make_async_remote_copy(
            src_ref=src, dst_ref=dst, send_sem=send, recv_sem=recv, device_id=target, device_id_type=MESH
        )

    def w_slot(chunk):
        start = node_of(chunk) * rows + chunk[3] * half
        return wg.at[pl.ds(pl.multiple_of(start, half), half)]

    def x_slot(chunk):
        start = node_of(chunk) * packed + chunk[3] * part_rows
        return xg.at[pl.ds(pl.multiple_of(start, 8), part_rows)]

    def a_slot(chunk):
        return rt.at[node_of(chunk)]

    def w_own(part):
        return w.at[pl.ds(part * half, half)]

    def x_own(part):
        return xpk.at[pl.ds(part * part_rows, part_rows)]

    phases = {
        "w": (two, w_slot, w_own, wsend, wrecv),
        "x": (early, x_slot, x_own, xsend, xrecv),
        "a": (one, a_slot, None, asend, arecv),
    }

    def send_copies(phase, k, value):
        rounds, slot, own, send, recv = phases[phase]
        copies = []
        for from_z, link, chunk in rounds[k]:
            if from_z != value:
                continue
            src = slot(chunk)
            if own is not None and chunk[:3] == (0, 0, value):
                src = own(chunk[3])
            copies.append(remote(src, slot(chunk), send.at[k // 4, link], recv.at[k, link], links[link]))
        return copies

    def recv_copies(phase, k, value):
        rounds, slot, _, send, recv = phases[phase]
        copies = []
        for act in rounds[k]:
            to, chunk = landed(act)
            if to == value:
                copies.append(remote(slot(chunk), slot(chunk), send.at[k // 4, act[1]], recv.at[k, act[1]], links[act[1]]))
        return copies

    def start(phase, k, value):
        for copy in send_copies(phase, k, value):
            copy.start()

    def arrive(phase, k, value):
        for copy in recv_copies(phase, k, value):
            copy.wait_recv()

    back = (0, 1, 3, 2)

    def reduce_moves(k, value):
        out, come = [], []
        for act in one[last_one - k]:
            to, chunk = landed(act)
            if to == value:
                out.append((back[act[1]], chunk))
            if act[0] == value:
                come.append((back[act[1]], act[2]))
        return out, come

    def reduce_copies(k, value):
        return [
            remote(zacc.at[node_of(chunk)], rsb.at[k, link], rsend.at[link], rrecv.at[k, link], links[link])
            for link, chunk in reduce_moves(k, value)[0]
        ]

    def reduce_start(k, value):
        for copy in reduce_copies(k, value):
            copy.start()

    def reduce_arrive(k, value):
        for link, chunk in reduce_moves(k, value)[1]:
            remote(rsb.at[k, link], rsb.at[k, link], rsend.at[link], rrecv.at[k, link], links[link]).wait_recv()
            owner = node_of(chunk)
            zacc[owner] = zacc[owner] + rsb[k, link]

    copy_panels = pltpu.make_async_copy(g.at[:, pl.ds(0, pair)], gpa, local.at[0])
    own_pair = pl.ds(pl.multiple_of((me // 2) * pair, LANE), pair)
    copy_diag = pltpu.make_async_copy(g.at[:, own_pair], gt.at[0], local.at[1])
    copy_w = pltpu.make_async_copy(w, wv, local.at[2])
    copy_diag.start()
    copy_panels.start()
    copy_w.start()
    copy_diag.wait()
    on_diag = iota((rows, pair), 1) == iota((rows, pair), 0) + rows * (me % 2)
    trace = jnp.sum(jnp.where(on_diag, gt[0], 0.0), keepdims=True)
    trown[...] = jnp.broadcast_to(trace, trown.shape)
    trs[me] = jnp.broadcast_to(trace, trown.shape)
    trace_copies = [
        remote(trown, trs.at[me], tsem.at[0], tsem.at[1], (t, (me + k) % nodes)) for k in range(1, nodes)
    ]
    for copy in trace_copies:
        copy.start()
    by_z(lambda v: start("w", 0, v))
    copy_panels.wait()
    gpv[0] = gpa[:, 0:rows]
    gpv[1] = gpa[:, rows:pair]
    others = trs.at[pl.ds(0, nodes - 1)]
    remote(others, others, tsem.at[0], tsem.at[1], partner).wait_recv()
    total = jnp.sum(trs[...], axis=0)[0:1, 0:1]
    scale = width / total
    sv[...] = jnp.broadcast_to(scale, sv.shape)

    def panel(which):
        raw = gpv[which]
        eye = (iota((rows, rows), 0) == iota((rows, rows), 1)) & (me == which)
        return scale * (0.9 * raw + jnp.where(eye, 0.1 * raw, 0.0))

    xs[...] = panel(1 - t)
    swap = remote(xs, xrv, dsend.at[0], drecv.at[0], partner)
    swap.start()
    xrp[t] = jnp.zeros(xrp.shape[1:], f32)
    swap.wait_recv()
    xrp[t, :, 0:rows] = panel(t) + xrv[...]
    share = remote(xrp.at[t], xrp.at[t], dsend.at[1], drecv.at[1], partner)
    share.start()
    for h in range(2):
        for j in range(3):
            xpk[(3 * h + j) * half : (3 * h + j + 1) * half, :] = xrp[t, h * half : (h + 1) * half, j * LANE : (j + 1) * LANE]
    xpk[6 * half : 7 * half, :] = xrp[t, 0:half, 3 * LANE : PAD] + pltpu.roll(
        xrp[t, half:rows, 3 * LANE : PAD], LANE // 2, 1
    )
    own_x = pl.ds(pl.multiple_of(me * packed, 8), packed)
    store_x = pltpu.make_async_copy(xpk, xg.at[own_x], local.at[3])
    store_x.start()
    copy_w.wait()
    own_rows = pl.ds(pl.multiple_of(me * rows, rows), rows)
    store_w = pltpu.make_async_copy(wv, wg.at[own_rows], local.at[4])
    store_w.start()
    by_z(lambda v: start("x", 0, v))

    def products(which, into):
        high, low = halves(panel(which))
        xh[0:rows, 0:rows] = high
        xl[0:rows, 0:rows] = low

        @pl.loop(0, columns // PAD)
        def _(c):
            part = wv[:, pl.ds(pl.multiple_of(c * PAD, PAD), PAD)]
            value = bf(xh[0:rows, 0:rows], part, TN) + bf(xl[0:rows, 0:rows], part, TN)
            for q in range(PAD // LANE):
                into[c * (PAD // LANE) + q] = value[:, q * LANE : (q + 1) * LANE]

    products(1 - t, zsend)
    trade = remote(zsend, zrecv, dsend.at[2], drecv.at[2], partner)
    trade.start()
    by_z(lambda v: (arrive("x", 0, v), start("x", 1, v)))
    products(t, zacc)
    trade.wait()

    @pl.loop(0, blocks)
    def _(i):
        zacc[i] = zacc[i] + zrecv[i]
        zsend[i] = jnp.zeros(zsend.shape[1:], f32)

    def own_top(v):
        reduce_arrive(last_one, v)
        rt[me] = zacc[me]
        start("a", 0, v)

    by_z(lambda v: (arrive("x", 1, v), start("x", 2, v), reduce_start(0, v)))
    size = cw.shape[0]
    same = iota((size, size), 0) == iota((size, size), 1)
    li[...] = jnp.where(same, 1.0, 0.0)
    cw[...] = jnp.where(same & (iota((size, size), 0) % PAD >= rows), 1.0, 0.0)
    share.wait()
    store_x.wait()
    store_w.wait()
    for k in range(3, 6):
        by_z(
            lambda v, k=k: (
                arrive("x", k - 1, v), start("x", k, v), reduce_arrive(k - 3, v), reduce_start(k - 2, v)
            )
        )

    by_z(lambda v: (arrive("x", 5, v), start("x", 6, v)))
    fetch = pltpu.make_async_copy(xg.at[pl.ds(0, 2 * packed)], xpm, local.at[5])
    fetch.start()
    fetch.wait()
    give = remote(xpm, xpo, dsend.at[3], drecv.at[3], partner)
    give.start()

    low_lanes = iota((half, LANE), 1) < LANE // 2

    def tile(ref, h, j):
        if j < 3:
            return ref[(3 * h + j) * half : (3 * h + j + 1) * half, :]
        last = ref[6 * half : 7 * half, :]
        if h == 1:
            last = pltpu.roll(last, LANE // 2, 1)
        return jnp.where(low_lanes, last, 0.0)

    def place(ref, which):
        for k in range(2):
            for h in range(2):
                for j in range(4):
                    at = pl.ds(pl.multiple_of(which * PAD + j * LANE, LANE), LANE)
                    cw[k * PAD + h * half : k * PAD + (h + 1) * half, at] = tile(ref.at[k * packed : (k + 1) * packed], h, j)

    place(xpm, t)
    give.wait()
    place(xpo, 1 - t)

    def eliminate(k):
        o = pl.multiple_of(k * LANE, LANE)
        step, wide = 16, 2 * LANE
        own = pl.ds(o, LANE)
        groups = LANE // step - (LANE // step // 2) * ((k % 4) // 3)
        sub, lane, sub1 = iota((LANE, LANE), 0), iota((LANE, LANE), 1), iota((LANE, 1), 0)
        sub8, lane8 = iota((step, LANE), 0), iota((step, LANE), 1)
        dref[...] = cw[own, own]
        bref[...] = jnp.where(sub == lane, 1.0, 0.0)

        def pivots(i, carry):
            at = pl.multiple_of(i * step, step)
            here = pl.ds(at, step)
            rows8 = dref[here, :]
            for s in range(step):
                column = jnp.sum(jnp.where(lane8 == at + s, rows8, 0.0), axis=1, keepdims=True)
                cref[s, 0:step, :] = jnp.broadcast_to(column, (step, LANE))
            scaled = []
            for s in range(step):
                inverse = 1.0 / cref[s, s : s + 1, :]
                factor = jnp.where(sub8 > s, cref[s, 0:step, :] * inverse, 0.0)
                for later in range(s + 1, step):
                    cref[later, 0:step, :] = cref[later, 0:step, :] - factor * cref[later, s : s + 1, :]
                row, brow = dref[pl.ds(at + s, 1), :], bref[pl.ds(at + s, 1), :]
                dref[here, :] = dref[here, :] - factor * row
                bref[here, :] = bref[here, :] - factor * brow
                scaled.append(row * inverse)
            factors = jnp.transpose(jnp.concatenate(scaled * (LANE // step), axis=0))
            d, b = dref[...], bref[...]
            for s in range(step):
                factor = jnp.where(sub1 >= at + step, factors[:, s : s + 1], 0.0)
                d = d - factor * dref[pl.ds(at + s, 1), :]
                b = b - factor * bref[pl.ds(at + s, 1), :]
            dref[...] = d
            bref[...] = b
            return carry

        lax.fori_loop(0, groups, pivots, 0)
        diagonal = jnp.sum(jnp.where(sub == lane, dref[...], 0.0), axis=1, keepdims=True)
        bref[...] = bref[...] * lax.rsqrt(diagonal)
        first = (o + LANE) // wide
        last = (o + LANE + wide - 1) // wide
        count = size // wide

        def finish(n, carry):
            at = pl.ds(pl.multiple_of(n * wide, wide), wide)
            li[own, at] = mm(bref[...], li[own, at])
            return carry

        def ahead(n, carry):
            at = pl.ds(pl.multiple_of(n * wide, wide), wide)
            uref[:, at] = mm(bref[...], cw[own, at])
            return carry

        lax.fori_loop(0, last, finish, 0)
        lax.fori_loop(first, count, ahead, 0)

        def below(i, carry):
            at = pl.ds(pl.multiple_of(i * LANE, LANE), LANE)
            dref[...] = jnp.transpose(uref[:, at])

            def right(n, carry):
                to = pl.ds(pl.multiple_of(n * wide, wide), wide)
                cw[at, to] = cw[at, to] - mm(dref[...], uref[:, to])
                return carry

            def left(n, carry):
                to = pl.ds(pl.multiple_of(n * wide, wide), wide)
                li[at, to] = li[at, to] - mm(dref[...], li[own, to])
                return carry

            lax.fori_loop(first, count, right, 0)
            lax.fori_loop(0, last, left, 0)
            return carry

        lax.fori_loop(k + 1, size // LANE, below, 0)

    def coefficients():
        wide = 2 * LANE

        @pl.loop(0, size // wide)
        def _(c):
            at = pl.ds(pl.multiple_of(c * wide, wide), wide)
            cw[0:rows, at] = mm(xrp[0], li[at, 0:PAD], NT) + mm(xrp[1], li[at, PAD:size], NT)

        top = pl.ds(pl.multiple_of(jnp.minimum(me, 1) * PAD, PAD), rows)

        @pl.loop(0, PAD // wide)
        def _(c):
            at = pl.ds(pl.multiple_of(t * PAD + c * wide, wide), wide)
            to = pl.ds(pl.multiple_of(c * wide, wide), wide)
            lower = -mm(cw[0:rows, :], li[:, at])
            value = jnp.where(me < PANEL_STEPS, li[top, at], lower)
            ahl[0:rows, to], ahl[rows:pair, to] = halves(value)

    def own_block(ref, j):
        raw = ref[...]
        eye = iota((rows, pair), 1) + j * pair == iota((rows, pair), 0) + me * rows
        return sv[0:1, 0:1] * (0.9 * raw + jnp.where(eye, 0.1 * raw, 0.0))

    def gram_tile(j, slot, sem):
        return pltpu.make_async_copy(g.at[:, pl.ds(pl.multiple_of(j * pair, LANE), pair)], gt.at[slot], sem)

    def gram_pieces():
        def load(j, slot):
            return (
                gram_tile(j, slot, elocal.at[slot, 0]),
                pltpu.make_async_copy(
                    xg.at[pl.ds(pl.multiple_of(2 * j * packed, 8), 2 * packed)], xp2.at[slot], elocal.at[slot, 1]
                ),
            )

        def out(j, slot):
            tile_out = cw.at[pl.ds(pl.multiple_of(slot * PAD, PAD), rows), pl.ds(0, pair)]
            at = pl.ds(pl.multiple_of(j * pair, LANE), pair)
            return (
                pltpu.make_async_copy(tile_out, em.at[:, at], elocal.at[slot, 2]),
                remote(tile_out, eo.at[:, at], esend.at[j], erecv.at[j], partner),
            )

        for copy in load(0, 0):
            copy.start()

        def piece(j, carry):
            slot = j % 2
            for copy in load(j, slot):
                copy.wait()

            @pl.when(j + 1 < blocks // 2)
            def _():
                for copy in load(j + 1, 1 - slot):
                    copy.start()

            @pl.when(j >= 2)
            def _():
                keep, away = out(j - 2, slot)
                keep.wait()
                away.wait()

            for k in range(2):
                for h in range(2):
                    at = slice(k * rows + h * half, k * rows + (h + 1) * half)
                    for q in range(4):
                        high, low = halves(tile(xp2.at[slot, k * packed : (k + 1) * packed], h, q))
                        xh[at, q * LANE : (q + 1) * LANE] = high
                        xl[at, q * LANE : (q + 1) * LANE] = low
            both = bf(ahl[...], xh[...], NT)
            value = both[0:rows] + (both[rows:pair] + bf(ahl[0:rows, :], xl[...], NT))
            value = value + jnp.where(me >= PANEL_STEPS, own_block(gt.at[slot], j), 0.0)
            cw[pl.ds(pl.multiple_of(slot * PAD, PAD), rows), pl.ds(0, pair)] = value
            keep, away = out(j, slot)
            keep.start()
            away.start()
            return carry

        lax.fori_loop(0, blocks // 2, piece, 0)
        for j in (blocks // 2 - 2, blocks // 2 - 1):
            keep, away = out(j, j % 2)
            keep.wait()
            away.wait()

    orders, ready = pair_order(two)

    def weight_piece(position, arrived=lambda: None):
        def pick(which):
            chosen = 0
            for p in range(SIDE * LINE):
                for v in range(LINE):
                    chosen = jnp.where((z == v) & (position == p), orders[v][p][which], chosen)
            return chosen

        b = pick(0)
        j = pick(1) * 2 + (y + b - 2 * b * y)
        final = isinstance(position, int)
        load = gram_tile(j, 0, local.at[6])
        load.start()
        load.wait()
        high, low = halves(jnp.where(me >= PANEL_STEPS, own_block(gt.at[0], j), 0.0))
        rhl[0:rows, :] = high
        rhl[rows:pair, :] = low
        arrived()
        rows_of = pl.ds(pl.multiple_of(j * pair, pair), pair)

        def part_copy(c):
            at = pl.ds(pl.multiple_of(c * PAD, PAD), PAD)
            return pltpu.make_async_copy(wg.at[rows_of, at], wt.at[c], wsem.at[c])

        for c in range(columns // PAD):
            part_copy(c).start()

        @pl.loop(0, columns // PAD)
        def _(c):
            part_copy(c).wait()
            both = bf(rhl[...], wt[c])
            value = both[0:rows] + both[rows:pair]
            for q in range(PAD // LANE):
                at = c * (PAD // LANE) + q
                piece = value[:, q * LANE : (q + 1) * LANE]
                zsend[at] = zsend[at] + piece
            if final:
                for copy in rhs_out(c):
                    copy.start()

    def weight_pieces(first, last):
        lax.fori_loop(first, last, lambda k, c: (weight_piece(k), c)[1], 0)

    def rhs_out(c):
        at = pl.ds(pl.multiple_of(c * (PAD // LANE), PAD // LANE), PAD // LANE)
        return (
            pltpu.make_async_copy(zsend.at[at], fm.at[at], flocal.at[c]),
            remote(zsend.at[at], fo.at[at], fsend.at[c], frecv.at[c], partner),
        )

    def top_share():
        @pl.loop(0, blocks)
        def _(i):
            high, low = halves(rt[i])
            both = bf(ahl[:, 0:rows], high)
            zsend[i] = zsend[i] + (both[0:rows] + (both[rows:pair] + bf(ahl[0:rows, 0:rows], low)))

    by_z(lambda v: (reduce_arrive(3, v), reduce_start(4, v), start("w", 1, v)))
    eliminate(0)
    by_z(lambda v: (arrive("x", 6, v), start("x", 7, v), own_top(v)))
    eliminate(1)
    by_z(lambda v: (arrive("x", 7, v), start("x", 8, v), arrive("a", 0, v), start("a", 1, v)))
    eliminate(2)
    by_z(lambda v: (arrive("x", 8, v), start("x", 9, v), arrive("a", 1, v), start("a", 2, v)))
    by_z(lambda v: (arrive("w", 0, v), start("w", 2, v)))
    lax.fori_loop(3, 5, lambda k, c: (eliminate(k), c)[1], 0)
    by_z(lambda v: (arrive("x", 9, v), arrive("a", 2, v), start("a", 3, v), arrive("w", 1, v), start("w", 3, v)))
    eliminate(5)
    by_z(lambda v: (arrive("a", 3, v), start("a", 4, v), arrive("w", 2, v), start("w", 4, v)))
    lax.fori_loop(6, 8, lambda k, c: (eliminate(k), c)[1], 0)
    by_z(lambda v: (arrive("w", 3, v), start("w", 5, v)))
    coefficients()
    gram_pieces()
    by_z(lambda v: (arrive("a", 4, v), arrive("w", 4, v), start("w", 6, v)))
    weight_pieces(0, 2)
    by_z(lambda v: (arrive("w", 5, v), start("w", 7, v)))
    weight_pieces(2, 3)
    top_share()
    by_z(lambda v: (arrive("w", 6, v), start("w", 8, v)))
    by_z(lambda v: (arrive("w", 7, v), start("w", 9, v)))
    weight_pieces(3, 5)
    by_z(lambda v: arrive("w", 8, v))
    weight_pieces(5, 7)
    weight_piece(7, lambda: by_z(lambda v: arrive("w", 9, v)))
    for c in range(columns // PAD):
        for copy in rhs_out(c):
            copy.wait()

    for copy in trace_copies[:1]:
        remote(others, others, tsem.at[0], tsem.at[1], partner).wait_send()
    swap.wait_send()

    def drained(v):
        for link in range(4):
            for name, rounds, whole, rows_each in (("w", two, wg, half), ("x", early, xg, part_rows), ("a", one, rt, 1)):
                for first in range(0, len(rounds), 4):
                    count = sum(act[0] == v and act[1] == link for acts in rounds[first : first + 4] for act in acts)
                    sem = phases[name][3].at[first // 4, link]
                    if count:
                        all_of = whole.at[pl.ds(0, count * rows_each)]
                        remote(all_of, all_of, sem, sem, partner).wait_send()
            count = sum(move[0] == link for k in range(len(one)) for move in reduce_moves(k, v)[0])
            if count:
                all_of = zacc.at[pl.ds(0, count)]
                remote(all_of, all_of, rsend.at[link], rsend.at[link], partner).wait_send()

    by_z(drained)


def fused(parts, activation_grams, adjusted_weights):
    f32, b16 = jnp.float32, jnp.bfloat16
    gram, weights = activation_grams[0], adjusted_weights[0]
    rows, width = gram.shape
    columns = weights.shape[1]
    half, blocks, size = rows // 2, columns // LANE, PANEL_STEPS * PAD
    packed = 7 * half
    hbm = pl.BlockSpec(memory_space=pl.ANY)
    vmem, dma = pltpu.VMEM, pltpu.SemaphoreType.DMA
    block = (blocks, rows, LANE)
    rounds, short = len(TWO), len(ONE)
    em, eo, fm, fo, _, _ = pl.pallas_call(
        kernel,
        out_shape=[
            jax.ShapeDtypeStruct((rows, width), f32),
            jax.ShapeDtypeStruct((rows, width), f32),
            jax.ShapeDtypeStruct(block, f32),
            jax.ShapeDtypeStruct(block, f32),
            jax.ShapeDtypeStruct((parts * rows, columns), b16),
            jax.ShapeDtypeStruct((parts * packed, LANE), f32),
        ],
        in_specs=[hbm] * 2,
        out_specs=[hbm] * 6,
        scratch_shapes=[
            vmem((rows, 2 * rows), f32), vmem((2, rows, rows), f32), vmem((2, rows, 2 * rows), f32), vmem((rows, columns), b16),
            vmem((8, LANE), f32), vmem((parts, 8, LANE), f32), vmem((8, LANE), f32),
            vmem((rows, rows), f32), vmem((rows, rows), f32), vmem((2, rows, PAD), f32), vmem((packed, LANE), f32),
            vmem(block, f32), vmem(block, f32), vmem(block, f32), vmem((short, 4, rows, LANE), f32), vmem(block, f32),
            vmem((size, size), f32), vmem((size, size), f32),
            vmem((2 * packed, LANE), f32), vmem((2 * packed, LANE), f32), vmem((2, 2 * packed, LANE), f32),
            vmem((LANE, LANE), f32), vmem((LANE, LANE), f32), vmem((16, 16, LANE), f32), vmem((LANE, size), f32),
            vmem((2 * rows, PAD), b16), vmem((2 * rows, PAD), b16), vmem((2 * rows, PAD), b16),
            vmem((2 * rows, 2 * rows), b16), vmem((columns // PAD, 2 * rows, PAD), b16),
            dma((3, 4)), dma((rounds, 4)), dma((3, 4)), dma((rounds, 4)),
            dma((4,)), dma((short, 4)), dma((2, 4)), dma((short, 4)),
            dma((9,)), dma((2,)), dma((4,)), dma((4,)), dma((8,)), dma((8,)), dma((2, 3)), dma((4,)), dma((4,)), dma((4,)), dma((4,)),
        ],
        compiler_params=pltpu.CompilerParams(has_side_effects=True, vmem_limit_bytes=67043328),
        name="merge",
    )(gram, weights)
    rhs = jnp.transpose(fm + fo, (1, 0, 2)).reshape(rows, columns)
    return em + eo, rhs


def product(left, right):
    return jnp.dot(left, right, precision=lax.Precision.HIGHEST)


def inverse_of(factor):
    identity = jnp.eye(factor.shape[0], dtype=factor.dtype)
    return jax.scipy.linalg.solve_triangular(factor, identity, lower=True)


def leading_block(columns_block, parts, rows, wide):
    position = lax.axis_index("row")
    holders = wide // rows
    if rows % parts == 0:
        pieces = lax.all_to_all(
            columns_block.reshape(parts, rows // parts, wide), "row", 0, 0, tiled=True
        )[:holders]
        gathered = lax.all_gather(pieces, "row", axis=1, tiled=True)
        return gathered.reshape(wide, wide)
    placed = jnp.zeros((wide, wide), columns_block.dtype)
    kept = jnp.where(position < holders, columns_block, 0)
    start = jnp.minimum(position, holders - 1) * rows
    return lax.psum(lax.dynamic_update_slice_in_dim(placed, kept, start, 0), "row")


def per_device(parts, activation_grams, adjusted_weights):
    gram = activation_grams[0]
    rows, width = gram.shape
    columns = adjusted_weights.shape[2]
    wide = PANEL_STEPS * rows
    position = lax.axis_index("row")
    task = lax.axis_index("task")
    start_col = position * rows
    weights = lax.all_gather(adjusted_weights[0], "row", axis=0, tiled=True)

    own_block = lax.dynamic_slice_in_dim(gram, start_col, rows, 1)
    diagonal_entries = jnp.diagonal(own_block)
    scaling = width / lax.psum(jnp.sum(diagonal_entries), "row")
    row_ids = lax.broadcasted_iota(jnp.int32, (rows, width), 0) + start_col
    col_ids = lax.broadcasted_iota(jnp.int32, (rows, width), 1)
    source = scaling * (0.9 * gram + jnp.where(row_ids == col_ids, 0.1 * gram, 0.0))

    panel_cols = lax.psum(source[:, :wide], "task")
    corner = leading_block(panel_cols, parts, rows, wide)
    first_inverse = inverse_of(jnp.linalg.cholesky(corner[:rows, :rows]))
    left = product(corner[rows:, :rows], first_inverse.T)
    second = jnp.linalg.cholesky(corner[rows:, rows:] - product(left, left.T))
    second_inverse = inverse_of(second)
    coupling = -product(second_inverse, product(left, first_inverse))
    solver = jnp.where(
        task == 0,
        jnp.concatenate([first_inverse, jnp.zeros_like(first_inverse)], axis=1),
        jnp.concatenate([coupling, second_inverse], axis=1),
    )
    mine = product(solver, panel_cols.T)
    upper = lax.all_gather(mine, "row", axis=1, tiled=True)

    high = lax.reduce_precision(source, 8, 7)
    low = (source - high).astype(jnp.bfloat16)
    folded = jnp.dot(
        high.astype(jnp.bfloat16), weights, preferred_element_type=jnp.float32
    ) + jnp.dot(low, weights, preferred_element_type=jnp.float32)

    pieces = lax.all_to_all(folded, "row", 1, 0, tiled=True)
    held, solver = lax.optimization_barrier((pieces[:wide], solver))
    top = lax.psum(held, "task")
    solved = lax.all_gather(product(solver, top), "row", axis=1, tiled=True)

    below = position >= PANEL_STEPS
    holds = position == task
    merged_part = jnp.where(
        below, source - product(mine.T, upper), jnp.where(holds, upper, 0.0)
    )
    rhs_part = jnp.where(
        below, folded - product(mine.T, solved), jnp.where(holds, solved, 0.0)
    )
    return lax.psum((merged_part, rhs_part), "task")


def solution(mesh):
    assert mesh.shape["task"] == PANEL_STEPS
    parts = mesh.shape["row"]
    placed = (P("task", "row", None), P("task", "row", None))

    def run(grams, weights):
        rows, columns = grams.shape[1], weights.shape[2]
        fits = parts == SIDE * SIDE * LINE and rows == 7 * LANE // 2 and columns == parts * LANE
        return (fused if fits else per_device)(parts, grams, weights)

    return jax.shard_map(
        run,
        mesh=mesh,
        in_specs=placed,
        out_specs=(P("row", None), P("row", None)),
        check_vma=False,
    )
```
